64 devices in a mesh: dp: 4 (over x, y), tp: 16 (over z, core).
Axes of the slice: x: 2, y: 2, z: 8, core: 2. Of those that a mesh axis runs over, the one named last changes fastest.
The devices are a block of a 4x4x8 slice.
Arguments:
- tokens: bfloat16 [4, 1024, 4096], P('dp', 'tp'), parts along dimension 0
- doc_ids: int32 [4, 1024], P('dp', 'tp'), parts along dimension 0
- norm1_gain: float32 [2, 4096], replicated
- norm1_shift: float32 [2, 4096], replicated
- qkv_weight: bfloat16 [2, 4096, 3, 16, 256], P(None, None, None, 'tp')
- out_weight: bfloat16 [2, 16, 256, 4096], P(None, 'tp')
- out_bias: float32 [2, 4096], replicated
- norm2_gain: float32 [2, 4096], replicated
- norm2_shift: float32 [2, 4096], replicated
- up_weight: bfloat16 [2, 4096, 16384], P(None, None, 'tp')
- up_bias: float32 [2, 16384], P(None, 'tp')
- down_weight: bfloat16 [2, 16384, 4096], P(None, 'tp')
- down_bias: float32 [2, 4096], replicated
Outputs:
- output: bfloat16 [4, 1024, 4096], P('dp', 'tp'), parts along dimension 0
There are 4 independent parts. The reference program is written for one: setup_inputs(seed, part) draws one part's arguments, and reference() takes and returns one part's arrays. A program takes and returns all parts, laid end to end along the dimension named above; an argument that names none is the same for every part.
All inputs are finite; a program needn't handle non-finite values.
Results may differ from the reference program's by a relative error of at most 0.0125964.
Values are sent between devices in bfloat16 or wider.
A program may use at most 768 MiB of HBM per device.

```python
import jax
import jax.numpy as jnp
from jax import lax

BATCH = 1
SEQ_LEN = 1024
D_MODEL = 4096
N_HEADS = 16
HEAD_DIM = 256
FF_DIM = 16384
GROUPS = 16
LAYERS = 2
DOC_CUTS = 3
QUERY_BLOCK = 256


def setup_inputs(seed: int = 0, part: int = 0) -> dict:
    root_key = jax.random.key(seed)
    keys_all = jax.random.split(root_key, 12)
    part_key = jax.random.fold_in(keys_all[0], part)
    tok_key, scale_key, cut_key = jax.random.split(part_key, 3)
    base_tok = jax.random.normal(tok_key, (BATCH, SEQ_LEN, D_MODEL), jnp.float32)
    row_scale = jnp.exp(0.5 * jax.random.normal(scale_key, (BATCH, SEQ_LEN, 1), jnp.float32))
    tokens = (base_tok * row_scale).astype(jnp.bfloat16)
    cut_pos = jax.random.randint(cut_key, (BATCH, 1, DOC_CUTS), 1, SEQ_LEN, dtype=jnp.int32)
    positions = jnp.arange(SEQ_LEN, dtype=jnp.int32)[None, :, None]
    doc_ids = jnp.sum((positions >= cut_pos).astype(jnp.int32), axis=-1, dtype=jnp.int32)
    d_scale = D_MODEL ** -0.5
    f_scale = FF_DIM ** -0.5
    qkv_mult = jnp.array([1.4142135, 1.4142135, 1.0], jnp.float32)[None, None, :, None, None]
    vec_shape = (LAYERS, D_MODEL)
    qkv_weight = jax.random.normal(keys_all[1], (LAYERS, D_MODEL, 3, N_HEADS, HEAD_DIM), jnp.float32) * qkv_mult * d_scale
    out_weight = jax.random.normal(keys_all[2], (LAYERS, N_HEADS, HEAD_DIM, D_MODEL), jnp.float32) * (1.5 * d_scale)
    up_weight = jax.random.normal(keys_all[3], (LAYERS, D_MODEL, FF_DIM), jnp.float32) * d_scale
    down_weight = jax.random.normal(keys_all[4], (LAYERS, FF_DIM, D_MODEL), jnp.float32) * f_scale
    return {
        "tokens": tokens,
        "doc_ids": doc_ids,
        "norm1_gain": 1.0 + 0.2 * jax.random.normal(keys_all[5], vec_shape, jnp.float32),
        "norm1_shift": 0.2 * jax.random.normal(keys_all[6], vec_shape, jnp.float32),
        "qkv_weight": qkv_weight.astype(jnp.bfloat16),
        "out_weight": out_weight.astype(jnp.bfloat16),
        "out_bias": 0.3 * jax.random.normal(keys_all[7], vec_shape, jnp.float32),
        "norm2_gain": 1.0 + 0.2 * jax.random.normal(keys_all[8], vec_shape, jnp.float32),
        "norm2_shift": 0.2 * jax.random.normal(keys_all[9], vec_shape, jnp.float32),
        "up_weight": up_weight.astype(jnp.bfloat16),
        "up_bias": 0.5 * jax.random.normal(keys_all[10], (LAYERS, FF_DIM), jnp.float32),
        "down_weight": down_weight.astype(jnp.bfloat16),
        "down_bias": 0.3 * jax.random.normal(keys_all[11], vec_shape, jnp.float32),
    }


def layer_norm(residual, gain_vec, shift_vec):
    mean_val = jnp.mean(residual, axis=-1, keepdims=True)
    centered = residual - mean_val
    variance = jnp.mean(centered * centered, axis=-1, keepdims=True)
    return (centered * lax.rsqrt(variance + 1e-5) * gain_vec + shift_vec).astype(jnp.bfloat16)


def attend_sequence(qkv_seq, ids_seq):
    n_blocks = SEQ_LEN // QUERY_BLOCK
    keys32 = qkv_seq[:, 1].astype(jnp.float32)
    values32 = qkv_seq[:, 2].astype(jnp.float32)
    q_blocks = qkv_seq[:, 0].reshape(n_blocks, QUERY_BLOCK, N_HEADS, HEAD_DIM)
    id_blocks = ids_seq.reshape(n_blocks, QUERY_BLOCK)
    starts = jnp.arange(n_blocks, dtype=jnp.int32) * QUERY_BLOCK
    key_pos = jnp.arange(SEQ_LEN, dtype=jnp.int32)

    def one_block(block_in):
        q_blk, id_blk, start_row = block_in
        scores = jnp.einsum("qhe,khe->hqk", q_blk.astype(jnp.float32), keys32) * (HEAD_DIM ** -0.5)
        query_pos = start_row + jnp.arange(QUERY_BLOCK, dtype=jnp.int32)
        allowed = (key_pos[None, :] <= query_pos[:, None]) & (ids_seq[None, :] == id_blk[:, None])
        scores = jnp.where(allowed[None], scores, -1e30)
        probs_blk = jax.nn.softmax(scores, axis=-1).astype(jnp.bfloat16)
        return jnp.einsum("hqk,khe->qhe", probs_blk.astype(jnp.float32), values32).astype(jnp.bfloat16)

    return lax.map(one_block, (q_blocks, id_blocks, starts)).reshape(SEQ_LEN, N_HEADS, HEAD_DIM)


def grouped_sum(activations, weight):
    def add_group(running, group_in):
        act_g, weight_g = group_in
        part_out = jnp.dot(act_g, weight_g, preferred_element_type=jnp.float32).astype(jnp.bfloat16)
        return running + part_out.astype(jnp.float32), None
    zero_acc = jnp.zeros((activations.shape[1], weight.shape[2]), jnp.float32)
    total, unused = lax.scan(add_group, zero_acc, (activations, weight))
    return total


def run_sequence(tok_seq, ids_seq, layer_params):
    head_group = N_HEADS // GROUPS
    ff_group = FF_DIM // GROUPS

    def one_layer(residual, params):
        n1_gain, n1_shift, w_qkv, w_out, b_out, n2_gain, n2_shift, w_up, b_up, w_down, b_down = params
        normed = layer_norm(residual, n1_gain, n1_shift)
        qkv_seq = jnp.dot(normed, w_qkv.reshape(D_MODEL, 3 * N_HEADS * HEAD_DIM), preferred_element_type=jnp.float32).astype(jnp.bfloat16)
        attn_out = attend_sequence(qkv_seq.reshape(SEQ_LEN, 3, N_HEADS, HEAD_DIM), ids_seq)
        attn_groups = jnp.moveaxis(attn_out.reshape(SEQ_LEN, GROUPS, head_group * HEAD_DIM), 1, 0)
        attn_sum = grouped_sum(attn_groups, w_out.reshape(GROUPS, head_group * HEAD_DIM, D_MODEL))
        residual = residual + (attn_sum + b_out)
        normed2 = layer_norm(residual, n2_gain, n2_shift)
        pre_act = jnp.dot(normed2, w_up, preferred_element_type=jnp.float32) + b_up
        hidden = jax.nn.gelu(pre_act, approximate=True).astype(jnp.bfloat16)
        hid_groups = jnp.moveaxis(hidden.reshape(SEQ_LEN, GROUPS, ff_group), 1, 0)
        mlp_sum = grouped_sum(hid_groups, w_down.reshape(GROUPS, ff_group, D_MODEL))
        residual = residual + (mlp_sum + b_down)
        return residual, None

    resid_end, unused = lax.scan(one_layer, tok_seq.astype(jnp.float32), layer_params)
    return resid_end.astype(jnp.bfloat16)


def reference(tokens, doc_ids, norm1_gain, norm1_shift, qkv_weight, out_weight, out_bias, norm2_gain, norm2_shift, up_weight, up_bias, down_weight, down_bias):
    layer_params = (norm1_gain, norm1_shift, qkv_weight, out_weight, out_bias, norm2_gain, norm2_shift, up_weight, up_bias, down_weight, down_bias)
    return lax.map(lambda seq_in: run_sequence(seq_in[0], seq_in[1], layer_params), (tokens, doc_ids))
```

```python
import jax
import jax.numpy as jnp
from jax import lax
from jax.sharding import PartitionSpec as P, NamedSharding

QUERY_ROWS = 512


def layer_norm(residual, gain_vec, shift_vec):
    mean_val = jnp.mean(residual, axis=-1, keepdims=True)
    centered = residual - mean_val
    variance = jnp.mean(centered * centered, axis=-1, keepdims=True)
    return (centered * lax.rsqrt(variance + 1e-5) * gain_vec + shift_vec).astype(jnp.bfloat16)


def doc_causal_attention(queries, keys_in, values_in, all_ids):
    seq_len = queries.shape[2]
    score_scale = queries.shape[3] ** -0.5
    block_rows = min(QUERY_ROWS, seq_len)
    pieces = []
    for start_row in range(0, seq_len, block_rows):
        stop_row = start_row + block_rows
        scores = jnp.einsum("bhqe,bhke->bhqk", queries[:, :, start_row:stop_row], keys_in[:, :, :stop_row], preferred_element_type=jnp.float32) * score_scale
        query_pos = start_row + jnp.arange(block_rows)
        key_pos = jnp.arange(stop_row)
        allowed = (key_pos[None, None, :] <= query_pos[None, :, None]) & (all_ids[:, start_row:stop_row, None] == all_ids[:, None, :stop_row])
        scores = jnp.where(allowed[:, None], scores, -1e30)
        probs_blk = jax.nn.softmax(scores, axis=-1).astype(jnp.bfloat16)
        pieces.append(jnp.einsum("bhqk,bhke->bqhe", probs_blk, values_in[:, :, :stop_row], preferred_element_type=jnp.float32).astype(jnp.bfloat16))
    return jnp.concatenate(pieces, axis=1)


def scatter_sum(partial_rows, groups):
    return lax.psum_scatter(partial_rows.astype(jnp.float32), "tp", scatter_dimension=1, tiled=True)


def solution(mesh):
    groups = mesh.shape["tp"]
    row_spec = P("dp", "tp", None)
    vec_spec = P(None, None)
    in_specs = (row_spec, P("dp", "tp"), vec_spec, vec_spec, P(None, None, None, "tp", None), P(None, "tp", None, None), vec_spec, vec_spec, vec_spec, P(None, None, "tp"), P(None, "tp"), P(None, "tp", None), vec_spec)

    def device_fn(tokens, doc_ids, norm1_gain, norm1_shift, qkv_weight, out_weight, out_bias, norm2_gain, norm2_shift, up_weight, up_bias, down_weight, down_bias):
        all_ids = lax.all_gather(doc_ids, "tp", axis=1, tiled=True)
        residual = tokens.astype(jnp.float32)
        for layer_idx in range(norm1_gain.shape[0]):
            normed = layer_norm(residual, norm1_gain[layer_idx], norm1_shift[layer_idx])
            full_rows = lax.all_gather(normed, "tp", axis=1, tiled=True)
            qkv_heads = jnp.einsum("bsd,dthe->tbhse", full_rows, qkv_weight[layer_idx], preferred_element_type=jnp.float32).astype(jnp.bfloat16)
            attn_out = doc_causal_attention(qkv_heads[0], qkv_heads[1], qkv_heads[2], all_ids)
            attn_part = jnp.einsum("bshe,hed->bsd", attn_out, out_weight[layer_idx], preferred_element_type=jnp.float32).astype(jnp.bfloat16)
            residual = residual + (scatter_sum(attn_part, groups) + out_bias[layer_idx])
            normed2 = layer_norm(residual, norm2_gain[layer_idx], norm2_shift[layer_idx])
            full_rows2 = lax.all_gather(normed2, "tp", axis=1, tiled=True)
            pre_act = jnp.einsum("bsd,df->bsf", full_rows2, up_weight[layer_idx], preferred_element_type=jnp.float32) + up_bias[layer_idx]
            hidden = jax.nn.gelu(pre_act, approximate=True).astype(jnp.bfloat16)
            mlp_part = jnp.einsum("bsf,fd->bsd", hidden, down_weight[layer_idx], preferred_element_type=jnp.float32).astype(jnp.bfloat16)
            residual = residual + (scatter_sum(mlp_part, groups) + down_bias[layer_idx])
        return residual.astype(jnp.bfloat16)

    return jax.shard_map(device_fn, mesh=mesh, in_specs=in_specs, out_specs=row_spec, check_vma=False)
```

```python
import functools

import jax
import jax.numpy as jnp
from jax import lax
from jax.experimental import pallas as pl
from jax.experimental.pallas import tpu as pltpu
from jax.sharding import PartitionSpec as P

MESH = pl.DeviceIdType.MESH
F32, BF16 = jnp.float32, jnp.bfloat16
ID_COLS = 128
RIGHT, LEFT = 0, 1


def loop(count, body):
    lax.fori_loop(0, count, lambda i, carry: (body(i), carry)[1], 0)


def cols_at(i, width):
    return pl.ds(pl.multiple_of(i * width, width), width)


def block_kernel(n, tokens_ref, ids_ref, g1_ref, s1_ref, ob_ref, g2_ref, s2_ref, ub_ref, db_ref, wqkv_hbm, wout_hbm, wup_hbm, wdown_hbm,
                 out_ref, hbuf, part, psib, ring, fresh, resid, wqkv, wout, wup, wdown, qkv, hidden, kpos, kids,
                 ag_send, ag_recv, sib_send, sib_recv, own_sem, part_send, part_recv, rs_send, rs_recv, w_sem, phase_sem):
    chips = n // 2
    far = chips // 2
    steps = 2 * far - 1
    layers = g1_ref.shape[0]
    rows, dim = tokens_ref.shape
    half_rows = rows // 2
    chip_rows = 2 * rows
    head = wout.shape[0]
    units = wup.shape[1]
    tile = min(512, dim)
    utile = min(512, units)

    me = lax.axis_index("tp")
    core = lax.rem(me, 2)
    chip = me // 2
    right, left = lax.rem(me + 2, n), lax.rem(me + n - 2, n)
    sibling = me + 1 - 2 * core
    target = (right, left)

    def slot_of(offset):
        if offset == 0:
            return 0
        if abs(offset) == far:
            return 1
        return 2 * abs(offset) + (1 if offset > 0 else 0)

    def signed(direction, distance):
        return -distance if direction == RIGHT else distance

    def ag_place(direction, m):
        distance = m // 2
        which = (m % 2) ^ direction
        return slot_of(signed(direction, distance)), slot_of(signed(direction, distance + 1)), pl.ds(which * half_rows, half_rows)

    def ag_copy(direction, m, width):
        src, dst, rws = ag_place(direction, m)
        return pltpu.make_async_remote_copy(
            src_ref=hbuf.at[src, core, rws, pl.ds(0, width)], dst_ref=hbuf.at[dst, core, rws, pl.ds(0, width)],
            send_sem=ag_send.at[direction, m], recv_sem=ag_recv.at[direction, m],
            device_id={"tp": target[direction]}, device_id_type=MESH)

    def sib_copy(direction, m, width):
        dst, rws = ag_place(direction, m)[1:]
        ref = hbuf.at[dst, core, rws, pl.ds(0, width)]
        return pltpu.make_async_remote_copy(
            src_ref=ref, dst_ref=ref, send_sem=sib_send.at[direction, m], recv_sem=sib_recv.at[direction, m],
            device_id={"tp": sibling}, device_id_type=MESH)

    def own_copy(width):
        ref = hbuf.at[0, core, pl.ds(0, rows), pl.ds(0, width)]
        return pltpu.make_async_remote_copy(
            src_ref=ref, dst_ref=ref, send_sem=own_sem.at[0], recv_sem=own_sem.at[1],
            device_id={"tp": sibling}, device_id_type=MESH)

    def part_copy(pair):
        return pltpu.make_async_remote_copy(
            src_ref=part.at[pl.ds(2 * pair, 2), 1 - core], dst_ref=psib.at[pl.ds(2 * pair, 2)],
            send_sem=part_send.at[pair], recv_sem=part_recv.at[pair],
            device_id={"tp": sibling}, device_id_type=MESH)

    def rs_plan(direction, m):
        if m == steps - 1:
            which, distance, before = 0, 1, m - 1
        elif m % 2 == 0:
            which, distance, before = 1, far - 1 - m // 2, m - 2
        else:
            which, distance, before = 0, far - m // 2, m - 2
        dest = slot_of(-signed(direction, distance))
        return which ^ direction, dest, (before if m >= 2 else None)

    def rs_copy(direction, m):
        before = rs_plan(direction, m)[2]
        src = fresh.at[direction, m] if before is None else ring.at[direction, before]
        return pltpu.make_async_remote_copy(
            src_ref=src, dst_ref=ring.at[direction, m], send_sem=rs_send.at[direction, m], recv_sem=rs_recv.at[direction, m],
            device_id={"tp": target[direction]}, device_id_type=MESH)

    def rs_step(m):
        for direction in (RIGHT, LEFT):
            which, dest, before = rs_plan(direction, m)
            if before is not None:
                rs_copy(direction, before).wait_recv()
            rws = pl.ds(which * half_rows, half_rows)

            def add(i):
                cs = cols_at(i, tile)
                total = part[dest, core, rws, cs].astype(F32) + psib[dest, rws, cs].astype(F32)
                if before is None:
                    fresh[direction, m, :, cs] = total
                else:
                    ring[direction, before, :, cs] = ring[direction, before, :, cs] + total

            loop(dim // tile, add)
            rs_copy(direction, m).start()

    def weight_copy(src, dst, index):
        return pltpu.make_async_copy(src, dst, w_sem.at[index])

    def signal_phase(sem):
        for device in (left, right, sibling):
            pl.semaphore_signal(sem, inc=1, device_id={"tp": device}, device_id_type=MESH)

    def norm(layer, gain_ref, shift_ref):
        for which in range(2):
            rws = pl.ds(which * half_rows, half_rows)

            def sum_body(i, acc):
                return acc + resid[rws, cols_at(i, tile)]

            total = lax.fori_loop(0, dim // tile, sum_body, jnp.zeros((half_rows, tile), F32))
            mean = jnp.sum(total, axis=1, keepdims=True) / dim

            def sq_body(i, acc):
                centered = resid[rws, cols_at(i, tile)] - mean
                return acc + centered * centered

            total = lax.fori_loop(0, dim // tile, sq_body, jnp.zeros((half_rows, tile), F32))
            scale = lax.rsqrt(jnp.sum(total, axis=1, keepdims=True) / dim + 1e-5)

            def out_body(i):
                cs = cols_at(i, tile)
                value = (resid[rws, cs] - mean) * scale * gain_ref[pl.ds(layer, 1), cs] + shift_ref[pl.ds(layer, 1), cs]
                hbuf[0, core, rws, cs] = value.astype(BF16)

            loop(dim // tile, out_body)

    def finish(layer, bias_ref):
        for which in range(2):
            last, early = (which, steps - 1), (1 - which, steps - 3)
            rs_copy(*early).wait_recv()
            rs_copy(*last).wait_recv()
            rws = pl.ds(which * half_rows, half_rows)

            def body(i):
                cs = cols_at(i, tile)
                total = part[0, core, rws, cs].astype(F32) + psib[0, rws, cs].astype(F32)
                total = total + ring[early[0], early[1], :, cs] + ring[last[0], last[1], :, cs]
                resid[rws, cs] = resid[rws, cs] + (total + bias_ref[pl.ds(layer, 1), cs])

            loop(dim // tile, body)
        for m in range(steps):
            for direction in (RIGHT, LEFT):
                rs_copy(direction, m).wait_send()
        for pair in range(far):
            part_copy(pair).wait_send()
        signal_phase(phase_sem)

    def pair_rows(pair):
        return hbuf[pl.ds(2 * pair, 2), :, :, pl.ds(0, dim)].reshape(2 * chip_rows, dim)

    def gather_start(width):
        for m in (0, 1):
            for direction in (RIGHT, LEFT):
                ag_copy(direction, m, width).start()
        own_copy(width).start()

    def gather_step(m, width):
        for direction in (RIGHT, LEFT):
            ag_copy(direction, m, width).wait_recv()
            if m + 2 < steps:
                ag_copy(direction, m + 2, width).start()
            sib_copy(direction, m, width).start()

    def sib_wait(m, width):
        for direction in (RIGHT, LEFT):
            sib_copy(direction, m, width).wait_recv()

    def gather_end(width):
        own_copy(width).wait_send()
        for m in range(steps):
            for direction in (RIGHT, LEFT):
                ag_copy(direction, m, width).wait_send()
                sib_copy(direction, m, width).wait_send()

    def exchange(width, first_half, second_half, prepare, finish_pair):
        gather_start(width)
        for m in range(steps):
            gather_step(m, width)
            if m % 2 == 1:
                sib_wait(m - 1, width)
                sib_wait(m, width)
                first_half(m // 2 + 1)
                if m == steps - 2:
                    second_half(far - 1)
            elif m >= 2 and m < steps - 1:
                second_half(m // 2)
        own_copy(width).wait_recv()
        prepare(steps - 1, width)
        finish_pair(far - 1)
        part_copy(far - 1).start()
        part_copy(far - 1).wait_recv()
        rs_step(0)

    def attention_half(layer):
        width = dim + ID_COLS

        def project(pair):
            lhs = pair_rows(pair)

            def body(t):
                value = jnp.dot(lhs, wqkv[t], preferred_element_type=F32).astype(BF16)
                qkv[t, pl.ds(2 * pair, 2)] = value.reshape(2, chip_rows, head)

            loop(3, body)

        def attend(pair):
            def body(i):
                slot = 2 * pair + i
                keys = qkv[1].reshape(chips * chip_rows, head)
                values = qkv[2].reshape(chips * chip_rows, head)
                scores = lax.dot_general(qkv[0, slot], keys, (((1,), (1,)), ((), ())), preferred_element_type=F32) * (head ** -0.5)
                ids_col = hbuf[slot, :, :, pl.ds(dim, ID_COLS)].astype(F32).reshape(chip_rows, ID_COLS)[:, 0:1]
                base = slot_chip(pair, i) * chip_rows
                pos_col = lax.broadcasted_iota(jnp.int32, (chip_rows, 1), 0) + base
                allowed = (kpos[0:1, :] <= pos_col) & (kids[0:1, :] == ids_col)
                scores = jnp.where(allowed, scores, -1e30)
                top = jnp.max(scores, axis=1, keepdims=True)
                probs = jnp.exp(scores - top)
                probs = (probs * (1.0 / jnp.sum(probs, axis=1, keepdims=True))).astype(BF16)
                mixed = jnp.dot(probs, values, preferred_element_type=F32).astype(BF16)

                def proj(c):
                    cs = cols_at(c, tile)
                    value = jnp.dot(mixed, wout[:, cs], preferred_element_type=F32).astype(BF16)
                    part[slot, :, :, cs] = value.reshape(2, rows, tile)

                loop(dim // tile, proj)

            loop(2, body)

        def slot_chip(pair, i):
            if pair == 0:
                return lax.rem(chip + i * far, chips)
            return lax.rem(chip + chips + (2 * i - 1) * pair, chips)

        def prepare(m, width):
            sib_wait(m, width)
            project(0)
            for pair in range(far):
                for i in range(2):
                    slot = 2 * pair + i
                    cs = pl.ds(slot * chip_rows, chip_rows)
                    kpos[:, cs] = lax.broadcasted_iota(jnp.int32, (8, chip_rows), 1) + slot_chip(pair, i) * chip_rows
                    block = hbuf[slot, :, :, pl.ds(dim, ID_COLS)].astype(F32).reshape(chip_rows, ID_COLS)
                    kids[:, cs] = block.T[0:8, :]

        weight_copy(wup_hbm.at[layer], wup, 2).start()
        weight_copy(wdown_hbm.at[layer], wdown, 3).start()
        weight_copy(wqkv_hbm.at[layer], wqkv, 0).wait()
        weight_copy(wout_hbm.at[layer], wout, 1).wait()
        exchange(width, project, lambda pair: None, prepare, attend)
        attend(0)
        part_copy(0).start()
        part_copy(0).wait_recv()
        rs_step(1)
        for pair in range(far - 2, 0, -1):
            attend(pair)
            part_copy(pair).start()
            part_copy(pair).wait_recv()
            first = 2 * (far - 1 - pair)
            rs_step(first)
            rs_step(first + 1)
        rs_step(steps - 1)
        gather_end(width)

    def mlp_half(layer):
        width = dim

        def up(pair):
            lhs = pair_rows(pair)

            def body(c):
                cs = cols_at(c, utile)
                x = jnp.dot(lhs, wup[:, cs], preferred_element_type=F32) + ub_ref[pl.ds(layer, 1), cs]
                inner = 0.7978845608028654 * (x + 0.044715 * (x * x * x))
                hidden[:, cs] = (0.5 * x * (1.0 + jnp.tanh(inner))).astype(BF16)

            loop(units // utile, body)

        def down(pair):
            def body(c):
                cs = cols_at(c, tile)
                value = jnp.dot(hidden[...], wdown[:, cs], preferred_element_type=F32).astype(BF16)
                part[pl.ds(2 * pair, 2), :, :, cs] = value.reshape(2, 2, rows, tile)

            loop(dim // tile, body)
            if pair != far - 1:
                part_copy(pair).start()

        weight_copy(wup_hbm.at[layer], wup, 2).wait()
        weight_copy(wdown_hbm.at[layer], wdown, 3).wait()

        @pl.when(layer + 1 < layers)
        def _():
            weight_copy(wqkv_hbm.at[layer + 1], wqkv, 0).start()
            weight_copy(wout_hbm.at[layer + 1], wout, 1).start()

        exchange(width, up, down, lambda m, width: None, lambda pair: None)
        sib_wait(steps - 1, width)
        up(0)
        down(0)
        part_copy(0).wait_recv()
        rs_step(1)
        for pair in range(far - 2, 0, -1):
            part_copy(pair).wait_recv()
            first = 2 * (far - 1 - pair)
            rs_step(first)
            rs_step(first + 1)
        rs_step(steps - 1)
        gather_end(width)

    weight_copy(wqkv_hbm.at[0], wqkv, 0).start()
    weight_copy(wout_hbm.at[0], wout, 1).start()
    barrier = pltpu.get_barrier_semaphore()
    signal_phase(barrier)
    for which in range(2):
        rws = pl.ds(which * half_rows, half_rows)
        loop(dim // tile, lambda i: resid.__setitem__((rws, cols_at(i, tile)), tokens_ref[rws, cols_at(i, tile)].astype(F32)))
    hbuf[0, core, :, pl.ds(dim, ID_COLS)] = ids_ref[...]
    norm(0, g1_ref, s1_ref)
    pl.semaphore_wait(barrier, 3)

    def layer_body(layer):
        attention_half(layer)
        finish(layer, ob_ref)
        norm(layer, g2_ref, s2_ref)
        pl.semaphore_wait(phase_sem, 3)
        mlp_half(layer)
        finish(layer, db_ref)
        norm(lax.rem(layer + 1, layers), g1_ref, s1_ref)
        pl.semaphore_wait(phase_sem, 3)

    loop(layers, layer_body)
    loop(dim // tile, lambda i: out_ref.__setitem__((slice(None), cols_at(i, tile)), resid[:, cols_at(i, tile)].astype(BF16)))


def solution(mesh):
    n = mesh.shape["tp"]
    chips = n // 2
    far = chips // 2
    steps = 2 * far - 1
    row_spec = P("dp", "tp", None)
    vec_spec = P(None, None)
    in_specs = (row_spec, P("dp", "tp"), vec_spec, vec_spec, P(None, None, None, "tp", None), P(None, "tp", None, None), vec_spec, vec_spec, vec_spec, P(None, None, "tp"), P(None, "tp"), P(None, "tp", None), vec_spec)

    def device_fn(tokens, doc_ids, norm1_gain, norm1_shift, qkv_weight, out_weight, out_bias, norm2_gain, norm2_shift, up_weight, up_bias, down_weight, down_bias):
        batch, rows, dim = tokens.shape
        layers = norm1_gain.shape[0]
        head = qkv_weight.shape[-1]
        units = up_weight.shape[-1]
        ids = jnp.broadcast_to(doc_ids.reshape(rows, 1).astype(BF16), (rows, ID_COLS))
        wqkv = jnp.transpose(qkv_weight, (0, 2, 3, 1, 4)).reshape(layers, 3, dim, head)
        wout = out_weight.reshape(layers, head, dim)
        vmem = pl.BlockSpec(memory_space=pltpu.VMEM)
        hbm = pl.BlockSpec(memory_space=pl.ANY)
        dma = pltpu.SemaphoreType.DMA
        result = pl.pallas_call(
            functools.partial(block_kernel, n),
            out_shape=jax.ShapeDtypeStruct((rows, dim), BF16),
            in_specs=[vmem] * 9 + [hbm] * 4,
            out_specs=vmem,
            scratch_shapes=[
                pltpu.VMEM((chips, 2, rows, dim + ID_COLS), BF16),
                pltpu.VMEM((chips, 2, rows, dim), BF16),
                pltpu.VMEM((chips, rows, dim), BF16),
                pltpu.VMEM((2, steps, rows // 2, dim), F32),
                pltpu.VMEM((2, 2, rows // 2, dim), F32),
                pltpu.VMEM((rows, dim), F32),
                pltpu.VMEM((3, dim, head), BF16),
                pltpu.VMEM((head, dim), BF16),
                pltpu.VMEM((dim, units), BF16),
                pltpu.VMEM((units, dim), BF16),
                pltpu.VMEM((3, chips, 2 * rows, head), BF16),
                pltpu.VMEM((4 * rows, units), BF16),
                pltpu.VMEM((8, chips * 2 * rows), jnp.int32),
                pltpu.VMEM((8, chips * 2 * rows), F32),
                dma((2, steps)), dma((2, steps)), dma((2, steps)), dma((2, steps)), dma((2,)),
                dma((far,)), dma((far,)), dma((2, steps)), dma((2, steps)), dma((4,)),
                pltpu.SemaphoreType.REGULAR,
            ],
            compiler_params=pltpu.CompilerParams(collective_id=0, has_side_effects=True, vmem_limit_bytes=67043328),
        )(tokens.reshape(rows, dim), ids, norm1_gain, norm1_shift, out_bias, norm2_gain, norm2_shift, up_bias, down_bias, wqkv, wout, up_weight, down_weight)
        return result.reshape(batch, rows, dim)

    return jax.shard_map(device_fn, mesh=mesh, in_specs=in_specs, out_specs=row_spec, check_vma=False)
```

```python
import functools

import jax
import jax.numpy as jnp
from jax import lax
from jax.experimental import pallas as pl
from jax.experimental.pallas import tpu as pltpu
from jax.sharding import PartitionSpec as P

MESH = pl.DeviceIdType.MESH
F32, BF16 = jnp.float32, jnp.bfloat16
ID_COLS = 128
RIGHT, LEFT = 0, 1


def loop(count, body):
    lax.fori_loop(0, count, lambda i, carry: (body(i), carry)[1], 0)


def cols_at(i, width):
    return pl.ds(pl.multiple_of(i * width, width), width)


def block_kernel(n, tokens_ref, ids_ref, g1_ref, s1_ref, ob_ref, g2_ref, s2_ref, ub_ref, db_ref, wqkv_hbm, wout_hbm, wup_hbm, wdown_hbm,
                 out_ref, hbuf, part, psib, ring, fresh, resid, wqkv, wout, wup, wdown, qkv, hidden, kpos, kids,
                 ag_send, ag_recv, sib_send, sib_recv, own_send, own_recv, part_send, part_recv, rs_send, rs_recv, w_sem):
    chips = n // 2
    far = chips // 2
    steps = 2 * far - 1
    layers = g1_ref.shape[0]
    rows, dim = tokens_ref.shape
    half_rows, quarter = rows // 2, rows // 4
    chip_rows = 2 * rows
    head = wout.shape[0]
    units = wup.shape[1]
    tile = min(512, dim)
    utile = min(512, units)

    me = lax.axis_index("tp")
    core = lax.rem(me, 2)
    chip = me // 2
    right, left = lax.rem(me + 2, n), lax.rem(me + n - 2, n)
    sibling = me + 1 - 2 * core
    target = (right, left)

    def slot_of(offset):
        if offset == 0:
            return 0
        if abs(offset) == far:
            return 1
        return 2 * abs(offset) + (1 if offset > 0 else 0)

    def slot_chip(slot):
        if slot == 0:
            return chip
        if slot == 1:
            return lax.rem(chip + far, chips)
        offset = slot // 2 if slot % 2 else -(slot // 2)
        return lax.rem(chip + chips + offset, chips)

    def signed(direction, distance):
        return -distance if direction == RIGHT else distance

    def quarter_rows(which, t):
        return pl.ds(which * half_rows + t * quarter, quarter)

    def half_ds(which):
        return pl.ds(which * half_rows, half_rows)

    def messages(direction):
        a, b = direction, 1 - direction
        out = [(0, a, 0), (0, b, 0), (0, a, 1), (0, b, 1)]
        for j in range(1, far - 1):
            out += [(j, a, 0), (j, a, 1), (j, b, 0), (j, b, 1)]
        return out + [(far - 1, a, 0), (far - 1, a, 1)]

    plans = (messages(RIGHT), messages(LEFT))
    count = len(plans[0])

    def width_of(which, t, with_ids):
        return dim + ID_COLS if with_ids and which == 0 and t == 0 else dim

    def ag_ref(direction, m, extra, with_ids):
        j, which, t = plans[direction][m]
        return hbuf.at[slot_of(signed(direction, j + extra)), core, quarter_rows(which, t), pl.ds(0, width_of(which, t, with_ids))]

    def ag_copy(direction, m, with_ids):
        return pltpu.make_async_remote_copy(
            src_ref=ag_ref(direction, m, 0, with_ids), dst_ref=ag_ref(direction, m, 1, with_ids),
            send_sem=ag_send.at[direction, m], recv_sem=ag_recv.at[direction, m],
            device_id={"tp": target[direction]}, device_id_type=MESH)

    def sib_copy(direction, m, with_ids):
        ref = ag_ref(direction, m, 1, with_ids)
        return pltpu.make_async_remote_copy(
            src_ref=ref, dst_ref=ref, send_sem=sib_send.at[direction, m], recv_sem=sib_recv.at[direction, m],
            device_id={"tp": sibling}, device_id_type=MESH)

    def own_copy(which, t, with_ids):
        ref = hbuf.at[0, core, quarter_rows(which, t), pl.ds(0, width_of(which, t, with_ids))]
        return pltpu.make_async_remote_copy(
            src_ref=ref, dst_ref=ref, send_sem=own_send.at[which, t], recv_sem=own_recv.at[which, t],
            device_id={"tp": sibling}, device_id_type=MESH)

    def part_copy(piece):
        slot, which = piece
        return pltpu.make_async_remote_copy(
            src_ref=part.at[slot, 1 - core, half_ds(which)], dst_ref=psib.at[slot, half_ds(which)],
            send_sem=part_send.at[slot, which], recv_sem=part_recv.at[slot, which],
            device_id={"tp": sibling}, device_id_type=MESH)

    def rs_plan(direction, m):
        if m == steps - 1:
            which, distance, before = 0, 1, m - 1
        elif m % 2 == 0:
            which, distance, before = 1, far - 1 - m // 2, m - 2
        else:
            which, distance, before = 0, far - m // 2, m - 2
        dest = slot_of(-signed(direction, distance))
        return which ^ direction, dest, (before if m >= 2 else None)

    def rs_copy(direction, m, t):
        before = rs_plan(direction, m)[2]
        src = fresh.at[direction, m, t] if before is None else ring.at[direction, before, t]
        return pltpu.make_async_remote_copy(
            src_ref=src, dst_ref=ring.at[direction, m, t], send_sem=rs_send.at[direction, m, t], recv_sem=rs_recv.at[direction, m, t],
            device_id={"tp": target[direction]}, device_id_type=MESH)

    def rs_step(m, need):
        for direction in (RIGHT, LEFT):
            which, dest, before = rs_plan(direction, m)
            need((dest, which))
        for t in range(2):
            for direction in (RIGHT, LEFT):
                which, dest, before = rs_plan(direction, m)
                if before is not None:
                    rs_copy(direction, before, t).wait_recv()
                rws = quarter_rows(which, t)

                def add(i):
                    cs = cols_at(i, tile)
                    total = part[dest, core, rws, cs].astype(F32) + psib[dest, rws, cs].astype(F32)
                    if before is None:
                        fresh[direction, m, t, :, cs] = total
                    else:
                        ring[direction, before, t, :, cs] = ring[direction, before, t, :, cs] + total

                loop(dim // tile, add)
                rs_copy(direction, m, t).start()

    def weight_copy(src, dst, index):
        return pltpu.make_async_copy(src, dst, w_sem.at[index])

    def norm_send(t, sums, layer, gain_ref, shift_ref, with_ids, before_send=None):
        means = [jnp.sum(s, axis=1, keepdims=True) / dim for s in sums]

        def sq_body(i, acc):
            out = []
            for which in range(2):
                centered = resid[quarter_rows(which, t), cols_at(i, tile)] - means[which]
                out.append(acc[which] + centered * centered)
            return tuple(out)

        zero = jnp.zeros((quarter, tile), F32)
        squares = lax.fori_loop(0, dim // tile, sq_body, (zero, zero))
        scales = [lax.rsqrt(jnp.sum(s, axis=1, keepdims=True) / dim + 1e-5) for s in squares]

        def out_body(i):
            cs = cols_at(i, tile)
            for which in range(2):
                rws = quarter_rows(which, t)
                value = (resid[rws, cs] - means[which]) * scales[which] * gain_ref[pl.ds(layer, 1), cs] + shift_ref[pl.ds(layer, 1), cs]
                hbuf[0, core, rws, cs] = value.astype(BF16)

        loop(dim // tile, out_body)
        if before_send is not None:
            before_send()
        for i in range(2):
            for direction in (RIGHT, LEFT):
                ag_copy(direction, 2 * t + i, with_ids).start()
        for which in range(2):
            own_copy(which, t, with_ids).start()

    def finish(t, layer, bias_ref):
        for which in range(2):
            rs_copy(1 - which, steps - 3, t).wait_recv()
            rs_copy(which, steps - 1, t).wait_recv()

        def body(i, acc):
            cs = cols_at(i, tile)
            out = []
            for which in range(2):
                rws = quarter_rows(which, t)
                total = part[0, core, rws, cs].astype(F32) + psib[0, rws, cs].astype(F32)
                total = total + ring[1 - which, steps - 3, t, :, cs] + ring[which, steps - 1, t, :, cs]
                value = resid[rws, cs] + (total + bias_ref[pl.ds(layer, 1), cs])
                resid[rws, cs] = value
                out.append(acc[which] + value)
            return tuple(out)

        zero = jnp.zeros((quarter, tile), F32)
        return lax.fori_loop(0, dim // tile, body, (zero, zero))

    def boundary(layer, bias_ref, next_layer, gain_ref, shift_ref, with_ids, more=None):
        for t in range(2):
            sums = finish(t, layer, bias_ref)
            if more is None:
                norm_send(t, sums, next_layer, gain_ref, shift_ref, with_ids)
            else:
                @pl.when(more)
                def _():
                    norm_send(t, sums, next_layer, gain_ref, shift_ref, with_ids)
        for m in range(steps):
            for direction in (RIGHT, LEFT):
                for t in range(2):
                    rs_copy(direction, m, t).wait_send()
        for slot in range(chips):
            for which in range(2):
                part_copy((slot, which)).wait_send()

    def needs():
        seen = set()

        def need(piece):
            if piece not in seen:
                seen.add(piece)
                part_copy(piece).wait_recv()

        return need

    def gather_step(m, with_ids):
        for direction in (RIGHT, LEFT):
            ag_copy(direction, m, with_ids).wait_recv()
            j, which, t = plans[direction][m]
            if (j + 1, which, t) in plans[direction]:
                ag_copy(direction, plans[direction].index((j + 1, which, t)), with_ids).start()
            sib_copy(direction, m, with_ids).start()

    def sib_wait(first, last, with_ids):
        for m in range(first, last + 1):
            for direction in (RIGHT, LEFT):
                sib_copy(direction, m, with_ids).wait_recv()

    def own_wait(with_ids):
        for which in range(2):
            for t in range(2):
                own_copy(which, t, with_ids).wait_recv()

    def gather_end(with_ids):
        for which in range(2):
            for t in range(2):
                own_copy(which, t, with_ids).wait_send()
        for m in range(count):
            for direction in (RIGHT, LEFT):
                ag_copy(direction, m, with_ids).wait_send()
                sib_copy(direction, m, with_ids).wait_send()

    def load_rows(pieces):
        return jnp.concatenate([hbuf[s, :, half_ds(w), pl.ds(0, dim)].reshape(rows, dim) for s, w in pieces], axis=0)

    def store_part(pieces, value, cs):
        for i, (s, w) in enumerate(pieces):
            part[s, :, half_ds(w), cs] = value[i * rows:(i + 1) * rows].reshape(2, half_rows, tile)

    def both(slot):
        return [(slot, 0), (slot, 1)]

    minus, plus = slot_of(-(far - 1)), slot_of(far - 1)
    own = both(0)
    farthest = both(1)
    leading = [(minus, 0), (plus, 1)]
    trailing = [(minus, 1), (plus, 0)]

    def near(p):
        return both(2 * p) + both(2 * p + 1)

    lead_at = 4 * (far - 2) + 1
    last_at = count - 1

    def send_parts(pieces):
        for piece in pieces:
            part_copy(piece).start()

    def attention_half(layer):
        need = needs()

        def project(pieces, kinds=(0, 3)):
            def body(t):
                value = jnp.dot(load_rows(pieces), wqkv[t], preferred_element_type=F32).astype(BF16)
                for i, (s, w) in enumerate(pieces):
                    qkv[t, s, :, half_ds(w)] = value[i * rows:(i + 1) * rows].reshape(2, half_rows, head)

            lax.fori_loop(kinds[0], kinds[1], lambda t, carry: (body(t), carry)[1], 0)

        def slot_ids(slot):
            cs = pl.ds(slot * chip_rows, chip_rows)
            lines = [hbuf[slot, c, pl.ds(0, 8), pl.ds(dim, ID_COLS)].astype(F32)[:, 0:rows] for c in range(2)]
            kids[:, cs] = jnp.concatenate(lines, axis=1)

        def column_ids(piece):
            slot, which = piece
            line = kids[0:1, pl.ds(slot * chip_rows, chip_rows)]
            column = jnp.broadcast_to(line, (chip_rows, chip_rows)).T[:, 0:1]
            return jnp.concatenate([column[c * rows + which * half_rows:c * rows + (which + 1) * half_rows] for c in range(2)], axis=0)

        def column_pos(piece):
            slot, which = piece
            i = lax.broadcasted_iota(jnp.int32, (rows, 1), 0)
            i = i + jnp.where(i >= half_rows, rows - half_rows, 0)
            return i + (which * half_rows + slot_chip(slot) * chip_rows)

        def attend(pieces):
            keys = qkv[1].reshape(chips * chip_rows, head)
            values = qkv[2].reshape(chips * chip_rows, head)
            queries = jnp.concatenate([qkv[0, s, :, half_ds(w)].reshape(rows, head) for s, w in pieces], axis=0)
            scores = lax.dot_general(queries, keys, (((1,), (1,)), ((), ())), preferred_element_type=F32) * (head ** -0.5)
            ids_col = jnp.concatenate([column_ids(piece) for piece in pieces], axis=0)
            pos_col = jnp.concatenate([column_pos(piece) for piece in pieces], axis=0)
            allowed = (kpos[0:1, :] <= pos_col) & (kids[0:1, :] == ids_col)
            scores = jnp.where(allowed, scores, -1e30)
            top = jnp.max(scores, axis=1, keepdims=True)
            probs = jnp.exp(scores - top)
            probs = (probs * (1.0 / jnp.sum(probs, axis=1, keepdims=True))).astype(BF16)
            mixed = jnp.dot(probs, values, preferred_element_type=F32).astype(BF16)

            def proj(c):
                cs = cols_at(c, tile)
                store_part(pieces, jnp.dot(mixed, wout[:, cs], preferred_element_type=F32).astype(BF16), cs)

            loop(dim // tile, proj)

        weight_copy(wup_hbm.at[layer], wup, 2).start()
        weight_copy(wdown_hbm.at[layer], wdown, 3).start()
        weight_copy(wqkv_hbm.at[layer], wqkv, 0).wait()
        weight_copy(wout_hbm.at[layer], wout, 1).wait()
        for m in range(count):
            gather_step(m, True)
            if m == 0:
                own_wait(True)
                project(own)
                slot_ids(0)
            for p in range(1, far - 1):
                if m == 4 * p:
                    sib_wait(4 * p - 4, 4 * p - 1, True)
                    project(near(p))
                    slot_ids(2 * p)
                    slot_ids(2 * p + 1)
            if m == last_at - 2:
                sib_wait(lead_at - 1, m, True)
                project(leading + trailing)
                slot_ids(minus)
                slot_ids(plus)
        sib_wait(last_at - 1, last_at, True)
        project(farthest, (1, 3))
        slot_ids(1)
        attend(leading)
        send_parts(leading)
        project(farthest, (0, 1))
        rs_step(0, need)
        attend(farthest)
        send_parts(farthest)
        rs_step(1, need)
        for pieces in [trailing] + [both(2 * p + i) for p in range(far - 2, 0, -1) for i in range(2)]:
            attend(pieces)
            send_parts(pieces)
        gather_end(True)
        attend(own)
        send_parts(own)
        for m in range(2, steps):
            rs_step(m, need)
        for piece in own:
            need(piece)

    def mlp_half(layer):
        need = needs()

        def up(pieces):
            count_rows = rows * len(pieces)

            def body(c):
                cs = cols_at(c, utile)
                x = jnp.dot(load_rows(pieces), wup[:, cs], preferred_element_type=F32) + ub_ref[pl.ds(layer, 1), cs]
                inner = 0.7978845608028654 * (x + 0.044715 * (x * x * x))
                hidden[pl.ds(0, count_rows), cs] = (0.5 * x * (1.0 + jnp.tanh(inner))).astype(BF16)

            loop(units // utile, body)

        def down(pieces):
            count_rows = rows * len(pieces)

            def body(c):
                cs = cols_at(c, tile)
                value = jnp.dot(hidden[pl.ds(0, count_rows), :], wdown[:, cs], preferred_element_type=F32).astype(BF16)
                store_part(pieces, value, cs)

            loop(dim // tile, body)

        weight_copy(wup_hbm.at[layer], wup, 2).wait()
        weight_copy(wdown_hbm.at[layer], wdown, 3).wait()

        @pl.when(layer + 1 < layers)
        def _():
            weight_copy(wqkv_hbm.at[layer + 1], wqkv, 0).start()
            weight_copy(wout_hbm.at[layer + 1], wout, 1).start()

        for m in range(last_at):
            gather_step(m, False)
            if m == 0:
                own_wait(False)
                up(own)
            if m == 1:
                down(own)
                send_parts(own)
            for p in range(1, far - 1):
                if m == 4 * p:
                    sib_wait(4 * p - 4, 4 * p - 1, False)
                    up(near(p))
                if m == 4 * p + (0 if p == far - 2 else 1):
                    down(near(p))
                    send_parts(near(p))
            if m == lead_at:
                sib_wait(lead_at - 1, lead_at, False)
                up(leading)
                down(leading)
                send_parts(leading)
        rs_step(0, need)
        gather_step(last_at, False)
        sib_wait(lead_at + 1, last_at, False)
        up(farthest + trailing)
        down(farthest + trailing)
        gather_end(False)
        send_parts(farthest + trailing)
        for m in range(1, steps):
            rs_step(m, need)
        for slot in range(chips):
            for piece in both(slot):
                need(piece)

    weight_copy(wqkv_hbm.at[0], wqkv, 0).start()
    weight_copy(wout_hbm.at[0], wout, 1).start()
    barrier = pltpu.get_barrier_semaphore()
    for device in (left, right, sibling):
        pl.semaphore_signal(barrier, inc=1, device_id={"tp": device}, device_id_type=MESH)
    hbuf[0, core, pl.ds(0, quarter), pl.ds(dim, ID_COLS)] = jnp.zeros((quarter, ID_COLS), BF16)
    hbuf[0, core, pl.ds(0, quarter), pl.ds(dim, rows)] = jnp.broadcast_to(ids_ref[...].astype(F32).astype(BF16), (quarter, rows))
    for slot in range(chips):
        kpos[:, pl.ds(slot * chip_rows, chip_rows)] = lax.broadcasted_iota(jnp.int32, (8, chip_rows), 1) + slot_chip(slot) * chip_rows
    for t in range(2):
        def widen(i, acc):
            out = []
            for which in range(2):
                rws = quarter_rows(which, t)
                value = tokens_ref[rws, cols_at(i, tile)].astype(F32)
                resid[rws, cols_at(i, tile)] = value
                out.append(acc[which] + value)
            return tuple(out)

        zero = jnp.zeros((quarter, tile), F32)
        sums = lax.fori_loop(0, dim // tile, widen, (zero, zero))
        norm_send(t, sums, 0, g1_ref, s1_ref, True, (lambda: pl.semaphore_wait(barrier, 3)) if t == 0 else None)

    def layer_body(layer):
        attention_half(layer)
        boundary(layer, ob_ref, layer, g2_ref, s2_ref, False)
        mlp_half(layer)
        boundary(layer, db_ref, lax.rem(layer + 1, layers), g1_ref, s1_ref, True, layer + 1 < layers)

    loop(layers, layer_body)
    loop(dim // tile, lambda i: out_ref.__setitem__((slice(None), cols_at(i, tile)), resid[:, cols_at(i, tile)].astype(BF16)))


def solution(mesh):
    n = mesh.shape["tp"]
    chips = n // 2
    far = chips // 2
    steps = 2 * far - 1
    sends = 4 * far - 2
    row_spec = P("dp", "tp", None)
    vec_spec = P(None, None)
    in_specs = (row_spec, P("dp", "tp"), vec_spec, vec_spec, P(None, None, None, "tp", None), P(None, "tp", None, None), vec_spec, vec_spec, vec_spec, P(None, None, "tp"), P(None, "tp"), P(None, "tp", None), vec_spec)

    def device_fn(tokens, doc_ids, norm1_gain, norm1_shift, qkv_weight, out_weight, out_bias, norm2_gain, norm2_shift, up_weight, up_bias, down_weight, down_bias):
        batch, rows, dim = tokens.shape
        layers = norm1_gain.shape[0]
        head = qkv_weight.shape[-1]
        units = up_weight.shape[-1]
        wqkv = jnp.transpose(qkv_weight, (0, 2, 3, 1, 4)).reshape(layers, 3, dim, head)
        wout = out_weight.reshape(layers, head, dim)
        vmem = pl.BlockSpec(memory_space=pltpu.VMEM)
        hbm = pl.BlockSpec(memory_space=pl.ANY)
        dma = pltpu.SemaphoreType.DMA
        result = pl.pallas_call(
            functools.partial(block_kernel, n),
            out_shape=jax.ShapeDtypeStruct((rows, dim), BF16),
            in_specs=[vmem] * 9 + [hbm] * 4,
            out_specs=vmem,
            scratch_shapes=[
                pltpu.VMEM((chips, 2, rows, dim + ID_COLS), BF16),
                pltpu.VMEM((chips, 2, rows, dim), BF16),
                pltpu.VMEM((chips, rows, dim), BF16),
                pltpu.VMEM((2, steps, 2, rows // 4, dim), F32),
                pltpu.VMEM((2, 2, 2, rows // 4, dim), F32),
                pltpu.VMEM((rows, dim), F32),
                pltpu.VMEM((3, dim, head), BF16),
                pltpu.VMEM((head, dim), BF16),
                pltpu.VMEM((dim, units), BF16),
                pltpu.VMEM((units, dim), BF16),
                pltpu.VMEM((3, chips, 2, rows, head), BF16),
                pltpu.VMEM((4 * rows, units), BF16),
                pltpu.VMEM((8, chips * 2 * rows), jnp.int32),
                pltpu.VMEM((8, chips * 2 * rows), F32),
                dma((2, sends)), dma((2, sends)), dma((2, sends)), dma((2, sends)), dma((2, 2)), dma((2, 2)),
                dma((chips, 2)), dma((chips, 2)), dma((2, steps, 2)), dma((2, steps, 2)), dma((4,)),
            ],
            compiler_params=pltpu.CompilerParams(collective_id=0, has_side_effects=True, vmem_limit_bytes=67043328),
        )(tokens.reshape(rows, dim), doc_ids, norm1_gain, norm1_shift, out_bias, norm2_gain, norm2_shift, up_bias, down_bias, wqkv, wout, up_weight, down_weight)
        return result.reshape(batch, rows, dim)

    return jax.shard_map(device_fn, mesh=mesh, in_specs=in_specs, out_specs=row_spec, check_vma=False)
```

```python
import functools

import jax
import jax.numpy as jnp
from jax import lax
from jax.experimental import pallas as pl
from jax.experimental.pallas import tpu as pltpu
from jax.sharding import PartitionSpec as P

MESH = pl.DeviceIdType.MESH
F32, BF16 = jnp.float32, jnp.bfloat16
ID_COLS = 128
RIGHT, LEFT = 0, 1


def loop(count, body):
    lax.fori_loop(0, count, lambda i, carry: (body(i), carry)[1], 0)


def cols_at(i, width):
    return pl.ds(pl.multiple_of(i * width, width), width)


def block_kernel(n, tokens_ref, ids_ref, g1_ref, s1_ref, ob_ref, g2_ref, s2_ref, ub_ref, db_ref, wqkv_hbm, wout_hbm, wup_hbm, wdown_hbm,
                 out_ref, hbuf, part, psib, ring, fresh, resid, wqkv, wout, wup, wdown, qkv, hidden, kpos, kids,
                 ag_send, ag_recv, sib_send, sib_recv, own_send, own_recv, part_send, part_recv, rs_send, rs_recv, w_sem):
    chips = n // 2
    far = chips // 2
    steps = 2 * far - 1
    layers = g1_ref.shape[0]
    rows, dim = tokens_ref.shape
    half_rows, quarter = rows // 2, rows // 4
    chip_rows = 2 * rows
    head = wout.shape[0]
    units = wup.shape[1]
    tile = min(512, dim)
    utile = min(512, units)
    wide = min(2048, dim)

    me = lax.axis_index("tp")
    core = lax.rem(me, 2)
    chip = me // 2
    right, left = lax.rem(me + 2, n), lax.rem(me + n - 2, n)
    sibling = me + 1 - 2 * core
    target = (right, left)

    def slot_of(offset):
        if offset == 0:
            return 0
        if abs(offset) == far:
            return 1
        return 2 * abs(offset) + (1 if offset > 0 else 0)

    def slot_chip(slot):
        if slot == 0:
            return chip
        if slot == 1:
            return lax.rem(chip + far, chips)
        offset = slot // 2 if slot % 2 else -(slot // 2)
        return lax.rem(chip + chips + offset, chips)

    def signed(direction, distance):
        return -distance if direction == RIGHT else distance

    def quarter_rows(which, t):
        return pl.ds(which * half_rows + t * quarter, quarter)

    def half_ds(which):
        return pl.ds(which * half_rows, half_rows)

    def messages(direction):
        a, b = direction, 1 - direction
        out = [(0, a, 0), (0, b, 0), (0, a, 1), (0, b, 1)]
        for j in range(1, far - 1):
            out += [(j, a, 0), (j, a, 1), (j, b, 0), (j, b, 1)]
        return out + [(far - 1, a, 0), (far - 1, a, 1)]

    plans = (messages(RIGHT), messages(LEFT))
    count = len(plans[0])

    def width_of(which, t, with_ids):
        return dim + ID_COLS if with_ids and which == 0 and t == 0 else dim

    def ag_ref(direction, m, extra, with_ids):
        j, which, t = plans[direction][m]
        return hbuf.at[slot_of(signed(direction, j + extra)), core, quarter_rows(which, t), pl.ds(0, width_of(which, t, with_ids))]

    def ag_copy(direction, m, with_ids):
        return pltpu.make_async_remote_copy(
            src_ref=ag_ref(direction, m, 0, with_ids), dst_ref=ag_ref(direction, m, 1, with_ids),
            send_sem=ag_send.at[direction, m], recv_sem=ag_recv.at[direction, m],
            device_id={"tp": target[direction]}, device_id_type=MESH)

    def sib_copy(direction, m, with_ids):
        ref = ag_ref(direction, m, 1, with_ids)
        return pltpu.make_async_remote_copy(
            src_ref=ref, dst_ref=ref, send_sem=sib_send.at[direction, m], recv_sem=sib_recv.at[direction, m],
            device_id={"tp": sibling}, device_id_type=MESH)

    def own_copy(which, t, with_ids):
        ref = hbuf.at[0, core, quarter_rows(which, t), pl.ds(0, width_of(which, t, with_ids))]
        return pltpu.make_async_remote_copy(
            src_ref=ref, dst_ref=ref, send_sem=own_send.at[which, t], recv_sem=own_recv.at[which, t],
            device_id={"tp": sibling}, device_id_type=MESH)

    def part_copy(slot, which, t):
        rws = quarter_rows(which, t)
        return pltpu.make_async_remote_copy(
            src_ref=part.at[slot, 1 - core, rws], dst_ref=psib.at[slot, rws],
            send_sem=part_send.at[slot, which, t], recv_sem=part_recv.at[slot, which, t],
            device_id={"tp": sibling}, device_id_type=MESH)

    def rs_plan(direction, m):
        if m == steps - 1:
            which, distance, before = 0, 1, m - 1
        elif m % 2 == 0:
            which, distance, before = 1, far - 1 - m // 2, m - 2
        else:
            which, distance, before = 0, far - m // 2, m - 2
        dest = slot_of(-signed(direction, distance))
        return which ^ direction, dest, (before if m >= 2 else None)

    def rs_copy(direction, m, t):
        before = rs_plan(direction, m)[2]
        src = fresh.at[direction, m, t] if before is None else ring.at[direction, before, t]
        return pltpu.make_async_remote_copy(
            src_ref=src, dst_ref=ring.at[direction, m, t], send_sem=rs_send.at[direction, m, t], recv_sem=rs_recv.at[direction, m, t],
            device_id={"tp": target[direction]}, device_id_type=MESH)

    def sum_send(m, t, need):
        for direction in (RIGHT, LEFT):
            which, dest, before = rs_plan(direction, m)
            need(dest, which, t)
            if before is not None:
                rs_copy(direction, before, t).wait_recv()
            rws = quarter_rows(which, t)

            def add(i):
                cs = cols_at(i, tile)
                total = part[dest, core, rws, cs].astype(F32) + psib[dest, rws, cs].astype(F32)
                if before is None:
                    fresh[direction, m, t, :, cs] = total
                else:
                    ring[direction, before, t, :, cs] = ring[direction, before, t, :, cs] + total

            loop(dim // tile, add)
            rs_copy(direction, m, t).start()

    def rs_step(m, need):
        for t in range(2):
            sum_send(m, t, need)

    def weight_copy(src, dst, index):
        return pltpu.make_async_copy(src, dst, w_sem.at[index])

    def norm_send(t, sums, layer, gain_ref, shift_ref, with_ids, before_send=None):
        means = [jnp.sum(s, axis=1, keepdims=True) / dim for s in sums]

        def sq_body(i, acc):
            out = []
            for which in range(2):
                centered = resid[quarter_rows(which, t), cols_at(i, tile)] - means[which]
                out.append(acc[which] + centered * centered)
            return tuple(out)

        zero = jnp.zeros((quarter, tile), F32)
        squares = lax.fori_loop(0, dim // tile, sq_body, (zero, zero))
        scales = [lax.rsqrt(jnp.sum(s, axis=1, keepdims=True) / dim + 1e-5) for s in squares]

        def out_body(i):
            cs = cols_at(i, tile)
            for which in range(2):
                rws = quarter_rows(which, t)
                value = (resid[rws, cs] - means[which]) * scales[which] * gain_ref[pl.ds(layer, 1), cs] + shift_ref[pl.ds(layer, 1), cs]
                hbuf[0, core, rws, cs] = value.astype(BF16)

        loop(dim // tile, out_body)
        if before_send is not None:
            before_send()
        for i in range(2):
            for direction in (RIGHT, LEFT):
                ag_copy(direction, 2 * t + i, with_ids).start()
        for which in range(2):
            own_copy(which, t, with_ids).start()

    def finish(t, layer, bias_ref):
        for which in range(2):
            rs_copy(1 - which, steps - 3, t).wait_recv()
            rs_copy(which, steps - 1, t).wait_recv()

        def body(i, acc):
            cs = cols_at(i, tile)
            out = []
            for which in range(2):
                rws = quarter_rows(which, t)
                total = part[0, core, rws, cs].astype(F32) + psib[0, rws, cs].astype(F32)
                total = total + ring[1 - which, steps - 3, t, :, cs] + ring[which, steps - 1, t, :, cs]
                value = resid[rws, cs] + (total + bias_ref[pl.ds(layer, 1), cs])
                resid[rws, cs] = value
                out_ref[rws, cs] = value.astype(BF16)
                out.append(acc[which] + value)
            return tuple(out)

        zero = jnp.zeros((quarter, tile), F32)
        return lax.fori_loop(0, dim // tile, body, (zero, zero))

    def boundary(layer, bias_ref, next_layer, gain_ref, shift_ref, with_ids, more=None):
        for t in range(2):
            sums = finish(t, layer, bias_ref)
            if more is None:
                norm_send(t, sums, next_layer, gain_ref, shift_ref, with_ids)
            else:
                @pl.when(more)
                def _():
                    norm_send(t, sums, next_layer, gain_ref, shift_ref, with_ids)
        for m in range(steps):
            for direction in (RIGHT, LEFT):
                for t in range(2):
                    rs_copy(direction, m, t).wait_send()
        for slot in range(chips):
            for which in range(2):
                for t in range(2):
                    part_copy(slot, which, t).wait_send()

    def needs():
        seen = set()

        def need(*piece):
            if piece not in seen:
                seen.add(piece)
                part_copy(*piece).wait_recv()

        return need

    def need_all(need):
        for slot in range(chips):
            for which in range(2):
                for t in range(2):
                    need(slot, which, t)

    def gather_step(m, with_ids):
        for direction in (RIGHT, LEFT):
            ag_copy(direction, m, with_ids).wait_recv()
            j, which, t = plans[direction][m]
            if (j + 1, which, t) in plans[direction]:
                ag_copy(direction, plans[direction].index((j + 1, which, t)), with_ids).start()
            sib_copy(direction, m, with_ids).start()

    def sib_wait(first, last, with_ids):
        for m in range(first, last + 1):
            for direction in (RIGHT, LEFT):
                sib_copy(direction, m, with_ids).wait_recv()

    def own_wait(with_ids):
        for which in range(2):
            for t in range(2):
                own_copy(which, t, with_ids).wait_recv()

    def gather_end(with_ids):
        for which in range(2):
            for t in range(2):
                own_copy(which, t, with_ids).wait_send()
        for m in range(count):
            for direction in (RIGHT, LEFT):
                ag_copy(direction, m, with_ids).wait_send()
                sib_copy(direction, m, with_ids).wait_send()

    def piece_rows(piece):
        slot, which, t = piece
        return half_ds(which) if t is None else quarter_rows(which, t)

    def piece_size(piece):
        return rows if piece[2] is None else half_rows

    def load_rows(pieces):
        return jnp.concatenate([hbuf[p[0], :, piece_rows(p), pl.ds(0, dim)].reshape(piece_size(p), dim) for p in pieces], axis=0)

    def store_part(pieces, value, cs):
        start = 0
        for p in pieces:
            size = piece_size(p)
            part[p[0], :, piece_rows(p), cs] = value[start:start + size].reshape(2, size // 2, value.shape[1])
            start += size

    def both(slot):
        return [(slot, 0, None), (slot, 1, None)]

    minus, plus = slot_of(-(far - 1)), slot_of(far - 1)
    own = both(0)
    farthest = both(1)
    leading = [(minus, 0, None), (plus, 1, None)]
    trailing = [(minus, 1, None), (plus, 0, None)]

    def near(p):
        return both(2 * p) + both(2 * p + 1)

    lead_at = 4 * (far - 2) + 1
    last_at = count - 1

    def send_parts(pieces):
        for slot, which, t in pieces:
            for u in range(2) if t is None else (t,):
                part_copy(slot, which, u).start()

    def attention_half(layer):
        need = needs()

        def project(pieces, kinds=(0, 3)):
            def body(t):
                value = jnp.dot(load_rows(pieces), wqkv[t], preferred_element_type=F32).astype(BF16)
                for i, p in enumerate(pieces):
                    qkv[t, p[0], :, piece_rows(p)] = value[i * rows:(i + 1) * rows].reshape(2, half_rows, head)

            lax.fori_loop(kinds[0], kinds[1], lambda t, carry: (body(t), carry)[1], 0)

        def slot_ids(slot):
            cs = pl.ds(slot * chip_rows, chip_rows)
            lines = [hbuf[slot, c, pl.ds(0, 8), pl.ds(dim, ID_COLS)].astype(F32)[:, 0:rows] for c in range(2)]
            kids[:, cs] = jnp.concatenate(lines, axis=1)

        def column_ids(piece):
            line = kids[0:1, pl.ds(piece[0] * chip_rows, chip_rows)]
            column = jnp.broadcast_to(line, (chip_rows, chip_rows)).T[:, 0:1]
            size = piece_size(piece) // 2
            first = piece[1] * half_rows + (piece[2] or 0) * quarter
            return jnp.concatenate([column[c * rows + first:c * rows + first + size] for c in range(2)], axis=0)

        def column_pos(piece):
            size = piece_size(piece) // 2
            first = piece[1] * half_rows + (piece[2] or 0) * quarter
            i = lax.broadcasted_iota(jnp.int32, (2 * size, 1), 0)
            i = i + jnp.where(i >= size, rows - size, 0)
            return i + (first + slot_chip(piece[0]) * chip_rows)

        def attend(pieces):
            keys = qkv[1].reshape(chips * chip_rows, head)
            values = qkv[2].reshape(chips * chip_rows, head)
            queries = jnp.concatenate([qkv[0, p[0], :, piece_rows(p)].reshape(piece_size(p), head) for p in pieces], axis=0)
            scores = lax.dot_general(queries, keys, (((1,), (1,)), ((), ())), preferred_element_type=F32) * (head ** -0.5)
            ids_col = jnp.concatenate([column_ids(piece) for piece in pieces], axis=0)
            pos_col = jnp.concatenate([column_pos(piece) for piece in pieces], axis=0)
            allowed = (kpos[0:1, :] <= pos_col) & (kids[0:1, :] == ids_col)
            scores = jnp.where(allowed, scores, -1e30)
            top = jnp.max(scores, axis=1, keepdims=True)
            probs = jnp.exp(scores - top)
            probs = (probs * (1.0 / jnp.sum(probs, axis=1, keepdims=True))).astype(BF16)
            mixed = jnp.dot(probs, values, preferred_element_type=F32).astype(BF16)

            def proj(c):
                cs = cols_at(c, wide)
                store_part(pieces, jnp.dot(mixed, wout[:, cs], preferred_element_type=F32).astype(BF16), cs)

            loop(dim // wide, proj)

        weight_copy(wup_hbm.at[layer], wup, 2).start()
        weight_copy(wdown_hbm.at[layer], wdown, 3).start()
        weight_copy(wqkv_hbm.at[layer], wqkv, 0).wait()
        weight_copy(wout_hbm.at[layer], wout, 1).wait()
        for m in range(count):
            gather_step(m, True)
            if m == 0:
                own_wait(True)
                project(own)
                slot_ids(0)
            for p in range(1, far - 1):
                if m == 4 * p:
                    sib_wait(4 * p - 4, 4 * p - 1, True)
                    project(near(p))
                    slot_ids(2 * p)
                    slot_ids(2 * p + 1)
            if m == last_at - 2:
                sib_wait(lead_at - 1, m, True)
                project(leading + trailing)
                slot_ids(minus)
                slot_ids(plus)
        sib_wait(last_at - 1, last_at, True)
        project(farthest, (1, 3))
        slot_ids(1)
        for t in range(2):
            quarters = [(slot, which, t) for slot, which, _ in leading]
            attend(quarters)
            send_parts(quarters)
        rs_step(0, need)
        project(farthest, (0, 1))
        attend(farthest)
        send_parts(farthest)
        rs_step(1, need)
        gather_end(True)
        attend(trailing)
        send_parts(trailing)
        for p in range(far - 2, 0, -1):
            for pieces in (both(2 * p), both(2 * p + 1)) + ((own,) if p == 1 else ()):
                attend(pieces)
                send_parts(pieces)
            rs_step(2 * (far - 1 - p), need)
            rs_step(2 * (far - 1 - p) + 1, need)
        rs_step(steps - 1, need)
        need_all(need)

    def mlp_half(layer):
        need = needs()

        def up(pieces):
            count_rows = rows * len(pieces)

            def body(c):
                cs = cols_at(c, utile)
                x = jnp.dot(load_rows(pieces), wup[:, cs], preferred_element_type=F32) + ub_ref[pl.ds(layer, 1), cs]
                inner = 0.7978845608028654 * (x + 0.044715 * (x * x * x))
                hidden[pl.ds(0, count_rows), cs] = (0.5 * x * (1.0 + jnp.tanh(inner))).astype(BF16)

            loop(units // utile, body)

        def down(pieces):
            count_rows = rows * len(pieces)
            step = min(wide, dim * 2 * rows // (2 * count_rows))

            def body(c):
                cs = cols_at(c, step)
                value = jnp.dot(hidden[pl.ds(0, count_rows), :], wdown[:, cs], preferred_element_type=F32).astype(BF16)
                store_part(pieces, value, cs)

            loop(dim // step, body)

        weight_copy(wup_hbm.at[layer], wup, 2).wait()
        weight_copy(wdown_hbm.at[layer], wdown, 3).wait()

        @pl.when(layer + 1 < layers)
        def _():
            weight_copy(wqkv_hbm.at[layer + 1], wqkv, 0).start()
            weight_copy(wout_hbm.at[layer + 1], wout, 1).start()

        for m in range(last_at):
            gather_step(m, False)
            if m == 0:
                own_wait(False)
                up(own)
            if m == 1:
                down(own)
                send_parts(own)
            for p in range(1, far - 2):
                if m == 4 * p:
                    sib_wait(4 * p - 4, 4 * p - 1, False)
                    up(near(p))
                if m == 4 * p + 1:
                    down(near(p))
                    send_parts(near(p))
            if m == lead_at:
                sib_wait(lead_at - 5, lead_at, False)
                up(leading)
                down(leading)
                send_parts(leading)
        rs_step(0, need)
        gather_step(last_at, False)
        sib_wait(lead_at + 1, last_at, False)
        up(farthest + trailing)
        down(farthest + trailing)
        send_parts(farthest + trailing)
        rs_step(1, need)
        gather_end(False)
        up(near(far - 2))
        down(near(far - 2))
        send_parts(near(far - 2))
        for m in range(2, steps):
            rs_step(m, need)
        need_all(need)

    weight_copy(wqkv_hbm.at[0], wqkv, 0).start()
    weight_copy(wout_hbm.at[0], wout, 1).start()
    barrier = pltpu.get_barrier_semaphore()
    for device in (left, right, sibling):
        pl.semaphore_signal(barrier, inc=1, device_id={"tp": device}, device_id_type=MESH)
    hbuf[0, core, pl.ds(0, quarter), pl.ds(dim, ID_COLS)] = jnp.zeros((quarter, ID_COLS), BF16)
    hbuf[0, core, pl.ds(0, quarter), pl.ds(dim, rows)] = jnp.broadcast_to(ids_ref[...].astype(F32).astype(BF16), (quarter, rows))
    for slot in range(chips):
        kpos[:, pl.ds(slot * chip_rows, chip_rows)] = lax.broadcasted_iota(jnp.int32, (8, chip_rows), 1) + slot_chip(slot) * chip_rows
    for t in range(2):
        def widen(i, acc):
            out = []
            for which in range(2):
                rws = quarter_rows(which, t)
                value = tokens_ref[rws, cols_at(i, tile)].astype(F32)
                resid[rws, cols_at(i, tile)] = value
                out.append(acc[which] + value)
            return tuple(out)

        zero = jnp.zeros((quarter, tile), F32)
        sums = lax.fori_loop(0, dim // tile, widen, (zero, zero))
        norm_send(t, sums, 0, g1_ref, s1_ref, True, (lambda: pl.semaphore_wait(barrier, 3)) if t == 0 else None)

    def layer_body(layer):
        attention_half(layer)
        boundary(layer, ob_ref, layer, g2_ref, s2_ref, False)
        mlp_half(layer)
        boundary(layer, db_ref, lax.rem(layer + 1, layers), g1_ref, s1_ref, True, layer + 1 < layers)

    loop(layers, layer_body)


def solution(mesh):
    n = mesh.shape["tp"]
    chips = n // 2
    far = chips // 2
    steps = 2 * far - 1
    sends = 4 * far - 2
    row_spec = P("dp", "tp", None)
    vec_spec = P(None, None)
    in_specs = (row_spec, P("dp", "tp"), vec_spec, vec_spec, P(None, None, None, "tp", None), P(None, "tp", None, None), vec_spec, vec_spec, vec_spec, P(None, None, "tp"), P(None, "tp"), P(None, "tp", None), vec_spec)

    def device_fn(tokens, doc_ids, norm1_gain, norm1_shift, qkv_weight, out_weight, out_bias, norm2_gain, norm2_shift, up_weight, up_bias, down_weight, down_bias):
        batch, rows, dim = tokens.shape
        layers = norm1_gain.shape[0]
        head = qkv_weight.shape[-1]
        units = up_weight.shape[-1]
        wqkv = jnp.transpose(qkv_weight, (0, 2, 3, 1, 4)).reshape(layers, 3, dim, head)
        wout = out_weight.reshape(layers, head, dim)
        vmem = pl.BlockSpec(memory_space=pltpu.VMEM)
        hbm = pl.BlockSpec(memory_space=pl.ANY)
        dma = pltpu.SemaphoreType.DMA
        result = pl.pallas_call(
            functools.partial(block_kernel, n),
            out_shape=jax.ShapeDtypeStruct((rows, dim), BF16),
            in_specs=[vmem] * 9 + [hbm] * 4,
            out_specs=vmem,
            scratch_shapes=[
                pltpu.VMEM((chips, 2, rows, dim + ID_COLS), BF16),
                pltpu.VMEM((chips, 2, rows, dim), BF16),
                pltpu.VMEM((chips, rows, dim), BF16),
                pltpu.VMEM((2, steps, 2, rows // 4, dim), F32),
                pltpu.VMEM((2, 2, 2, rows // 4, dim), F32),
                pltpu.VMEM((rows, dim), F32),
                pltpu.VMEM((3, dim, head), BF16),
                pltpu.VMEM((head, dim), BF16),
                pltpu.VMEM((dim, units), BF16),
                pltpu.VMEM((units, dim), BF16),
                pltpu.VMEM((3, chips, 2, rows, head), BF16),
                pltpu.VMEM((4 * rows, units), BF16),
                pltpu.VMEM((8, chips * 2 * rows), jnp.int32),
                pltpu.VMEM((8, chips * 2 * rows), F32),
                dma((2, sends)), dma((2, sends)), dma((2, sends)), dma((2, sends)), dma((2, 2)), dma((2, 2)),
                dma((chips, 2, 2)), dma((chips, 2, 2)), dma((2, steps, 2)), dma((2, steps, 2)), dma((4,)),
            ],
            compiler_params=pltpu.CompilerParams(collective_id=0, has_side_effects=True, vmem_limit_bytes=67043328),
        )(tokens.reshape(rows, dim), doc_ids, norm1_gain, norm1_shift, out_bias, norm2_gain, norm2_shift, up_bias, down_bias, wqkv, wout, up_weight, down_weight)
        return result.reshape(batch, rows, dim)

    return jax.shard_map(device_fn, mesh=mesh, in_specs=in_specs, out_specs=row_spec, check_vma=False)
```

```python
import functools

import jax
import jax.numpy as jnp
from jax import lax
from jax.experimental import pallas as pl
from jax.experimental.pallas import tpu as pltpu
from jax.sharding import PartitionSpec as P

MESH = pl.DeviceIdType.MESH
F32, BF16 = jnp.float32, jnp.bfloat16
ID_COLS = 128
RIGHT, LEFT = 0, 1


def loop(count, body):
    lax.fori_loop(0, count, lambda i, carry: (body(i), carry)[1], 0)


def cols_at(i, width):
    return pl.ds(pl.multiple_of(i * width, width), width)


def block_kernel(n, tokens_ref, ids_ref, g1_ref, s1_ref, ob_ref, g2_ref, s2_ref, ub_ref, db_ref, wqkv_hbm, wout_hbm, wup_hbm, wdown_hbm,
                 resid, hbuf, part, psib, ring, fresh, lead, wqkv, wout, wup, wdown, qkv, hidden, kpos, kids,
                 ag_send, ag_recv, sib_send, sib_recv, own_send, own_recv, part_send, part_recv, rs_send, rs_recv, lead_send, lead_recv, w_sem):
    chips = n // 2
    far = chips // 2
    steps = 2 * far - 1
    layers = g1_ref.shape[0]
    rows, dim = tokens_ref.shape
    half_rows, quarter = rows // 2, rows // 4
    chip_rows = 2 * rows
    head = wout.shape[0]
    units = wup.shape[1]
    tile = min(512, dim)
    utile = min(512, units)
    wide = min(2048, dim)

    me = lax.axis_index("tp")
    core = lax.rem(me, 2)
    chip = me // 2
    right, left = lax.rem(me + 2, n), lax.rem(me + n - 2, n)
    sibling = me + 1 - 2 * core
    target = (right, left)
    crossed = (right + 1 - 2 * core, left + 1 - 2 * core)

    def slot_of(offset):
        if offset == 0:
            return 0
        if abs(offset) == far:
            return 1
        return 2 * abs(offset) + (1 if offset > 0 else 0)

    def slot_chip(slot):
        if slot == 0:
            return chip
        if slot == 1:
            return lax.rem(chip + far, chips)
        offset = slot // 2 if slot % 2 else -(slot // 2)
        return lax.rem(chip + chips + offset, chips)

    def signed(direction, distance):
        return -distance if direction == RIGHT else distance

    def quarter_rows(which, t):
        return pl.ds(which * half_rows + t * quarter, quarter)

    def half_ds(which):
        return pl.ds(which * half_rows, half_rows)

    def messages(direction):
        a, b = direction, 1 - direction
        out = [(0, a, 0), (0, b, 0), (0, a, 1), (0, b, 1)]
        for j in range(1, far - 1):
            out += [(j, a, 0), (j, a, 1), (j, b, 0), (j, b, 1)]
        return out + [(far - 1, a, 0), (far - 1, a, 1)]

    plans = (messages(RIGHT), messages(LEFT))
    count = len(plans[0])

    def width_of(which, t, with_ids):
        return dim + ID_COLS if with_ids and which == 0 and t == 0 else dim

    def ag_ref(direction, m, extra, with_ids):
        j, which, t = plans[direction][m]
        return hbuf.at[slot_of(signed(direction, j + extra)), core, quarter_rows(which, t), pl.ds(0, width_of(which, t, with_ids))]

    def ag_copy(direction, m, with_ids):
        return pltpu.make_async_remote_copy(
            src_ref=ag_ref(direction, m, 0, with_ids), dst_ref=ag_ref(direction, m, 1, with_ids),
            send_sem=ag_send.at[direction, m], recv_sem=ag_recv.at[direction, m],
            device_id={"tp": target[direction]}, device_id_type=MESH)

    def sib_copy(direction, m, with_ids):
        ref = ag_ref(direction, m, 1, with_ids)
        return pltpu.make_async_remote_copy(
            src_ref=ref, dst_ref=ref, send_sem=sib_send.at[direction, m], recv_sem=sib_recv.at[direction, m],
            device_id={"tp": sibling}, device_id_type=MESH)

    def own_copy(which, t, with_ids):
        ref = hbuf.at[0, core, quarter_rows(which, t), pl.ds(0, width_of(which, t, with_ids))]
        return pltpu.make_async_remote_copy(
            src_ref=ref, dst_ref=ref, send_sem=own_send.at[which, t], recv_sem=own_recv.at[which, t],
            device_id={"tp": sibling}, device_id_type=MESH)

    def part_copy(slot, which, t):
        rws = quarter_rows(which, t)
        return pltpu.make_async_remote_copy(
            src_ref=part.at[slot, 1 - core, rws], dst_ref=psib.at[slot, rws],
            send_sem=part_send.at[slot, which, t], recv_sem=part_recv.at[slot, which, t],
            device_id={"tp": sibling}, device_id_type=MESH)

    def rs_plan(direction, m):
        if m == steps - 1:
            which, distance, before = 0, 1, m - 1
        elif m % 2 == 0:
            which, distance, before = 1, far - 1 - m // 2, m - 2
        else:
            which, distance, before = 0, far - m // 2, m - 2
        dest = slot_of(-signed(direction, distance))
        return which ^ direction, dest, (before if m >= 2 else None)

    def rs_copy(direction, m, t):
        before = rs_plan(direction, m)[2]
        src = fresh.at[direction, t] if before is None else ring.at[direction, before, t]
        return pltpu.make_async_remote_copy(
            src_ref=src, dst_ref=ring.at[direction, m, t], send_sem=rs_send.at[direction, m, t], recv_sem=rs_recv.at[direction, m, t],
            device_id={"tp": target[direction]}, device_id_type=MESH)

    def lead_copy(direction, t, cross):
        which, dest, _ = rs_plan(direction, 0)
        return pltpu.make_async_remote_copy(
            src_ref=part.at[dest, 1 - core if cross else core, quarter_rows(which, t)], dst_ref=lead.at[direction, t, cross],
            send_sem=lead_send.at[direction, t, cross], recv_sem=lead_recv.at[direction, t, cross],
            device_id={"tp": (crossed if cross else target)[direction]}, device_id_type=MESH)

    def lead_send_all(t):
        for cross in (0, 1):
            for direction in (RIGHT, LEFT):
                lead_copy(direction, t, cross).start()

    def sum_send(m, t, need):
        for direction in (RIGHT, LEFT):
            which, dest, before = rs_plan(direction, m)
            need(dest, which, t)
            if before == 0:
                for cross in (0, 1):
                    lead_copy(direction, t, cross).wait_recv()
            elif before is not None:
                rs_copy(direction, before, t).wait_recv()
            rws = quarter_rows(which, t)

            def add(i):
                cs = cols_at(i, tile)
                total = part[dest, core, rws, cs].astype(F32) + psib[dest, rws, cs].astype(F32)
                if before is None:
                    fresh[direction, t, :, cs] = total
                elif before == 0:
                    first = lead[direction, t, 0, :, cs].astype(F32) + lead[direction, t, 1, :, cs].astype(F32)
                    ring[direction, 0, t, :, cs] = first + total
                else:
                    ring[direction, before, t, :, cs] = ring[direction, before, t, :, cs] + total

            loop(dim // tile, add)
            rs_copy(direction, m, t).start()

    def rs_step(m, need):
        for t in range(2):
            sum_send(m, t, need)

    def weight_copy(src, dst, index):
        return pltpu.make_async_copy(src, dst, w_sem.at[index])

    def norm_send(t, sums, layer, gain_ref, shift_ref, with_ids, before_send=None):
        means = [jnp.sum(s, axis=1, keepdims=True) / dim for s in sums]

        def sq_body(i, acc):
            out = []
            for which in range(2):
                centered = resid[quarter_rows(which, t), cols_at(i, tile)] - means[which]
                out.append(acc[which] + centered * centered)
            return tuple(out)

        zero = jnp.zeros((quarter, tile), F32)
        squares = lax.fori_loop(0, dim // tile, sq_body, (zero, zero))
        scales = [lax.rsqrt(jnp.sum(s, axis=1, keepdims=True) / dim + 1e-5) for s in squares]

        def out_body(i):
            cs = cols_at(i, tile)
            for which in range(2):
                rws = quarter_rows(which, t)
                value = (resid[rws, cs] - means[which]) * scales[which] * gain_ref[pl.ds(layer, 1), cs] + shift_ref[pl.ds(layer, 1), cs]
                hbuf[0, core, rws, cs] = value.astype(BF16)

        loop(dim // tile, out_body)
        if before_send is not None:
            before_send()
        for i in range(2):
            for direction in (RIGHT, LEFT):
                ag_copy(direction, 2 * t + i, with_ids).start()
        for which in range(2):
            own_copy(which, t, with_ids).start()

    def finish(t, layer, bias_ref):
        for which in range(2):
            rs_copy(1 - which, steps - 3, t).wait_recv()
            rs_copy(which, steps - 1, t).wait_recv()

        def body(i, acc):
            cs = cols_at(i, tile)
            out = []
            for which in range(2):
                rws = quarter_rows(which, t)
                total = part[0, core, rws, cs].astype(F32) + psib[0, rws, cs].astype(F32)
                total = total + ring[1 - which, steps - 3, t, :, cs] + ring[which, steps - 1, t, :, cs]
                value = resid[rws, cs] + (total + bias_ref[pl.ds(layer, 1), cs])
                resid[rws, cs] = value
                out.append(acc[which] + value)
            return tuple(out)

        zero = jnp.zeros((quarter, tile), F32)
        return lax.fori_loop(0, dim // tile, body, (zero, zero))

    def boundary(layer, bias_ref, next_layer, gain_ref, shift_ref, with_ids, more=None):
        for t in range(2):
            sums = finish(t, layer, bias_ref)
            if more is None:
                norm_send(t, sums, next_layer, gain_ref, shift_ref, with_ids)
            else:
                @pl.when(more)
                def _():
                    norm_send(t, sums, next_layer, gain_ref, shift_ref, with_ids)
        for direction in (RIGHT, LEFT):
            for t in range(2):
                for cross in (0, 1):
                    lead_copy(direction, t, cross).wait_send()
                for m in range(1, steps):
                    rs_copy(direction, m, t).wait_send()
        for piece in exchanged:
            part_copy(*piece).wait_send()

    def needs():
        seen = set()

        def need(*piece):
            if piece not in seen:
                seen.add(piece)
                part_copy(*piece).wait_recv()

        return need

    def need_all(need):
        for piece in exchanged:
            need(*piece)

    def gather_step(m, with_ids):
        for direction in (RIGHT, LEFT):
            ag_copy(direction, m, with_ids).wait_recv()
            j, which, t = plans[direction][m]
            if (j + 1, which, t) in plans[direction]:
                ag_copy(direction, plans[direction].index((j + 1, which, t)), with_ids).start()
            sib_copy(direction, m, with_ids).start()

    def sib_wait(first, last, with_ids):
        for m in range(first, last + 1):
            for direction in (RIGHT, LEFT):
                sib_copy(direction, m, with_ids).wait_recv()

    def own_wait(with_ids):
        for which in range(2):
            for t in range(2):
                own_copy(which, t, with_ids).wait_recv()

    def gather_end(with_ids):
        for which in range(2):
            for t in range(2):
                own_copy(which, t, with_ids).wait_send()
        for m in range(count):
            for direction in (RIGHT, LEFT):
                ag_copy(direction, m, with_ids).wait_send()
                sib_copy(direction, m, with_ids).wait_send()

    def piece_rows(piece):
        slot, which, t = piece
        return half_ds(which) if t is None else quarter_rows(which, t)

    def piece_size(piece):
        return rows if piece[2] is None else half_rows

    def load_rows(pieces):
        return jnp.concatenate([hbuf[p[0], :, piece_rows(p), pl.ds(0, dim)].reshape(piece_size(p), dim) for p in pieces], axis=0)

    def store_part(pieces, value, cs):
        start = 0
        for p in pieces:
            size = piece_size(p)
            part[p[0], :, piece_rows(p), cs] = value[start:start + size].reshape(2, size // 2, value.shape[1])
            start += size

    def both(slot):
        return [(slot, 0, None), (slot, 1, None)]

    minus, plus = slot_of(-(far - 1)), slot_of(far - 1)
    own = both(0)
    farthest = both(1)
    leading = [(minus, 0, None), (plus, 1, None)]
    trailing = [(minus, 1, None), (plus, 0, None)]

    exchanged = [(slot, which, t) for slot in range(chips) for which in range(2) for t in range(2) if (slot, which, None) not in leading]

    def near(p):
        return both(2 * p) + both(2 * p + 1)

    lead_at = 4 * (far - 2) + 1
    last_at = count - 1

    def send_parts(pieces):
        for slot, which, t in pieces:
            for u in range(2) if t is None else (t,):
                part_copy(slot, which, u).start()

    def attention_half(layer):
        need = needs()

        def project(pieces, kinds=(0, 3)):
            def body(t):
                value = jnp.dot(load_rows(pieces), wqkv[t], preferred_element_type=F32).astype(BF16)
                for i, p in enumerate(pieces):
                    qkv[t, p[0], :, piece_rows(p)] = value[i * rows:(i + 1) * rows].reshape(2, half_rows, head)

            lax.fori_loop(kinds[0], kinds[1], lambda t, carry: (body(t), carry)[1], 0)

        def slot_ids(slot):
            cs = pl.ds(slot * chip_rows, chip_rows)
            lines = [hbuf[slot, c, pl.ds(0, 8), pl.ds(dim, ID_COLS)].astype(F32)[:, 0:rows] for c in range(2)]
            kids[:, cs] = jnp.concatenate(lines, axis=1)

        def column_ids(piece):
            line = kids[0:1, pl.ds(piece[0] * chip_rows, chip_rows)]
            column = jnp.broadcast_to(line, (chip_rows, chip_rows)).T[:, 0:1]
            size = piece_size(piece) // 2
            first = piece[1] * half_rows + (piece[2] or 0) * quarter
            return jnp.concatenate([column[c * rows + first:c * rows + first + size] for c in range(2)], axis=0)

        def column_pos(piece):
            size = piece_size(piece) // 2
            first = piece[1] * half_rows + (piece[2] or 0) * quarter
            i = lax.broadcasted_iota(jnp.int32, (2 * size, 1), 0)
            i = i + jnp.where(i >= size, rows - size, 0)
            return i + (first + slot_chip(piece[0]) * chip_rows)

        def attend(pieces):
            keys = qkv[1].reshape(chips * chip_rows, head)
            values = qkv[2].reshape(chips * chip_rows, head)
            queries = jnp.concatenate([qkv[0, p[0], :, piece_rows(p)].reshape(piece_size(p), head) for p in pieces], axis=0)
            scores = lax.dot_general(queries, keys, (((1,), (1,)), ((), ())), preferred_element_type=F32) * (head ** -0.5)
            ids_col = jnp.concatenate([column_ids(piece) for piece in pieces], axis=0)
            pos_col = jnp.concatenate([column_pos(piece) for piece in pieces], axis=0)
            allowed = (kpos[0:1, :] <= pos_col) & (kids[0:1, :] == ids_col)
            scores = jnp.where(allowed, scores, -1e30)
            top = jnp.max(scores, axis=1, keepdims=True)
            probs = jnp.exp(scores - top)
            probs = (probs * (1.0 / jnp.sum(probs, axis=1, keepdims=True))).astype(BF16)
            mixed = jnp.dot(probs, values, preferred_element_type=F32).astype(BF16)

            def proj(c):
                cs = cols_at(c, wide)
                store_part(pieces, jnp.dot(mixed, wout[:, cs], preferred_element_type=F32).astype(BF16), cs)

            loop(dim // wide, proj)

        weight_copy(wup_hbm.at[layer], wup, 2).start()
        weight_copy(wdown_hbm.at[layer], wdown, 3).start()
        weight_copy(wqkv_hbm.at[layer], wqkv, 0).wait()
        weight_copy(wout_hbm.at[layer], wout, 1).wait()
        for m in range(count):
            gather_step(m, True)
            if m == 0:
                own_wait(True)
                project(own)
                slot_ids(0)
            for p in range(1, far - 1):
                if m == 4 * p:
                    sib_wait(4 * p - 4, 4 * p - 1, True)
                    project(near(p))
                    slot_ids(2 * p)
                    slot_ids(2 * p + 1)
            if m == last_at - 2:
                sib_wait(lead_at - 1, m, True)
                project(leading + trailing)
                slot_ids(minus)
                slot_ids(plus)
        sib_wait(last_at - 1, last_at, True)
        project(farthest, (1, 3))
        slot_ids(1)
        for t in range(2):
            quarters = [(slot, which, t) for slot, which, _ in leading]
            attend(quarters)
            lead_send_all(t)
        project(farthest, (0, 1))
        attend(farthest)
        send_parts(farthest)
        rs_step(1, need)
        gather_end(True)
        attend(trailing)
        send_parts(trailing)
        for p in range(far - 2, 0, -1):
            for pieces in (both(2 * p), both(2 * p + 1)) + ((own,) if p == 1 else ()):
                attend(pieces)
                send_parts(pieces)
            rs_step(2 * (far - 1 - p), need)
            rs_step(2 * (far - 1 - p) + 1, need)
        rs_step(steps - 1, need)
        need_all(need)

    def mlp_half(layer):
        need = needs()

        def up(pieces):
            count_rows = rows * len(pieces)

            def body(c):
                cs = cols_at(c, utile)
                x = jnp.dot(load_rows(pieces), wup[:, cs], preferred_element_type=F32) + ub_ref[pl.ds(layer, 1), cs]
                inner = 0.7978845608028654 * (x + 0.044715 * (x * x * x))
                hidden[pl.ds(0, count_rows), cs] = (0.5 * x * (1.0 + jnp.tanh(inner))).astype(BF16)

            loop(units // utile, body)

        def down(pieces):
            count_rows = rows * len(pieces)
            step = min(wide, dim * 2 * rows // (2 * count_rows))

            def body(c):
                cs = cols_at(c, step)
                value = jnp.dot(hidden[pl.ds(0, count_rows), :], wdown[:, cs], preferred_element_type=F32).astype(BF16)
                store_part(pieces, value, cs)

            loop(dim // step, body)

        weight_copy(wup_hbm.at[layer], wup, 2).wait()
        weight_copy(wdown_hbm.at[layer], wdown, 3).wait()

        @pl.when(layer + 1 < layers)
        def _():
            weight_copy(wqkv_hbm.at[layer + 1], wqkv, 0).start()
            weight_copy(wout_hbm.at[layer + 1], wout, 1).start()

        for m in range(last_at):
            gather_step(m, False)
            if m == 0:
                own_wait(False)
                up(own)
            if m == 1:
                down(own)
                send_parts(own)
            for p in range(1, far - 2):
                if m == 4 * p:
                    sib_wait(4 * p - 4, 4 * p - 1, False)
                    up(near(p))
                if m == 4 * p + 1:
                    down(near(p))
                    send_parts(near(p))
            if m == lead_at:
                sib_wait(lead_at - 5, lead_at, False)
                up(leading)
                down(leading)
                for t in range(2):
                    lead_send_all(t)
        gather_step(last_at, False)
        sib_wait(lead_at + 1, last_at, False)
        up(farthest + trailing)
        down(farthest + trailing)
        send_parts(farthest + trailing)
        rs_step(1, need)
        gather_end(False)
        up(near(far - 2))
        down(near(far - 2))
        send_parts(near(far - 2))
        for m in range(2, steps):
            rs_step(m, need)
        need_all(need)

    weight_copy(wqkv_hbm.at[0], wqkv, 0).start()
    weight_copy(wout_hbm.at[0], wout, 1).start()
    barrier = pltpu.get_barrier_semaphore()
    for device in (left, right, sibling) + crossed:
        pl.semaphore_signal(barrier, inc=1, device_id={"tp": device}, device_id_type=MESH)
    hbuf[0, core, pl.ds(0, quarter), pl.ds(dim, ID_COLS)] = jnp.zeros((quarter, ID_COLS), BF16)
    hbuf[0, core, pl.ds(0, quarter), pl.ds(dim, rows)] = jnp.broadcast_to(ids_ref[...].astype(F32).astype(BF16), (quarter, rows))
    for slot in range(chips):
        kpos[:, pl.ds(slot * chip_rows, chip_rows)] = lax.broadcasted_iota(jnp.int32, (8, chip_rows), 1) + slot_chip(slot) * chip_rows
    for t in range(2):
        def widen(i, acc):
            out = []
            for which in range(2):
                rws = quarter_rows(which, t)
                value = tokens_ref[rws, cols_at(i, tile)].astype(F32)
                resid[rws, cols_at(i, tile)] = value
                out.append(acc[which] + value)
            return tuple(out)

        zero = jnp.zeros((quarter, tile), F32)
        sums = lax.fori_loop(0, dim // tile, widen, (zero, zero))
        norm_send(t, sums, 0, g1_ref, s1_ref, True, (lambda: pl.semaphore_wait(barrier, 5)) if t == 0 else None)

    def layer_body(layer):
        attention_half(layer)
        boundary(layer, ob_ref, layer, g2_ref, s2_ref, False)
        mlp_half(layer)
        boundary(layer, db_ref, lax.rem(layer + 1, layers), g1_ref, s1_ref, True, layer + 1 < layers)

    loop(layers, layer_body)


def solution(mesh):
    n = mesh.shape["tp"]
    chips = n // 2
    far = chips // 2
    steps = 2 * far - 1
    sends = 4 * far - 2
    row_spec = P("dp", "tp", None)
    vec_spec = P(None, None)
    in_specs = (row_spec, P("dp", "tp"), vec_spec, vec_spec, P(None, None, None, "tp", None), P(None, "tp", None, None), vec_spec, vec_spec, vec_spec, P(None, None, "tp"), P(None, "tp"), P(None, "tp", None), vec_spec)

    def device_fn(tokens, doc_ids, norm1_gain, norm1_shift, qkv_weight, out_weight, out_bias, norm2_gain, norm2_shift, up_weight, up_bias, down_weight, down_bias):
        batch, rows, dim = tokens.shape
        layers = norm1_gain.shape[0]
        head = qkv_weight.shape[-1]
        units = up_weight.shape[-1]
        wqkv = jnp.transpose(qkv_weight, (0, 2, 3, 1, 4)).reshape(layers, 3, dim, head)
        wout = out_weight.reshape(layers, head, dim)
        vmem = pl.BlockSpec(memory_space=pltpu.VMEM)
        hbm = pl.BlockSpec(memory_space=pl.ANY)
        dma = pltpu.SemaphoreType.DMA
        result = pl.pallas_call(
            functools.partial(block_kernel, n),
            out_shape=jax.ShapeDtypeStruct((rows, dim), F32),
            in_specs=[vmem] * 9 + [hbm] * 4,
            out_specs=vmem,
            scratch_shapes=[
                pltpu.VMEM((chips, 2, rows, dim + ID_COLS), BF16),
                pltpu.VMEM((chips, 2, rows, dim), BF16),
                pltpu.VMEM((chips, rows, dim), BF16),
                pltpu.VMEM((2, steps, 2, rows // 4, dim), F32),
                pltpu.VMEM((2, 2, rows // 4, dim), F32),
                pltpu.VMEM((2, 2, 2, rows // 4, dim), BF16),
                pltpu.VMEM((3, dim, head), BF16),
                pltpu.VMEM((head, dim), BF16),
                pltpu.VMEM((dim, units), BF16),
                pltpu.VMEM((units, dim), BF16),
                pltpu.VMEM((3, chips, 2, rows, head), BF16),
                pltpu.VMEM((4 * rows, units), BF16),
                pltpu.VMEM((8, chips * 2 * rows), jnp.int32),
                pltpu.VMEM((8, chips * 2 * rows), F32),
                dma((2, sends)), dma((2, sends)), dma((2, sends)), dma((2, sends)), dma((2, 2)), dma((2, 2)),
                dma((chips, 2, 2)), dma((chips, 2, 2)), dma((2, steps, 2)), dma((2, steps, 2)), dma((2, 2, 2)), dma((2, 2, 2)), dma((4,)),
            ],
            compiler_params=pltpu.CompilerParams(collective_id=0, has_side_effects=True, vmem_limit_bytes=67043328),
        )(tokens.reshape(rows, dim), doc_ids, norm1_gain, norm1_shift, out_bias, norm2_gain, norm2_shift, up_bias, down_bias, wqkv, wout, up_weight, down_weight)
        return result.astype(BF16).reshape(batch, rows, dim)

    return jax.shard_map(device_fn, mesh=mesh, in_specs=in_specs, out_specs=row_spec, check_vma=False)
```

```python
import functools

import jax
import jax.numpy as jnp
from jax import lax
from jax.experimental import pallas as pl
from jax.experimental.pallas import tpu as pltpu
from jax.sharding import PartitionSpec as P

MESH = pl.DeviceIdType.MESH
F32, BF16 = jnp.float32, jnp.bfloat16
ID_COLS = 128
RIGHT, LEFT = 0, 1


def loop(count, body):
    lax.fori_loop(0, count, lambda i, carry: (body(i), carry)[1], 0)


def cols_at(i, width):
    return pl.ds(pl.multiple_of(i * width, width), width)


def block_kernel(n, tokens_ref, ids_ref, g1_ref, s1_ref, ob_ref, g2_ref, s2_ref, ub_ref, db_ref, wqkv_hbm, wout_hbm, wup_hbm, wdown_hbm,
                 out_ref, hbuf, part, psib, ring, fresh, lead, resid, wqkv, wout, wup, wdown, qkv, hidden, kpos, kids,
                 ag_send, ag_recv, sib_send, sib_recv, own_send, own_recv, part_send, part_recv, rs_send, rs_recv, lead_send, lead_recv, w_sem):
    chips = n // 2
    far = chips // 2
    steps = 2 * far - 1
    layers = g1_ref.shape[0]
    rows, dim = tokens_ref.shape
    half_rows, quarter = rows // 2, rows // 4
    chip_rows = 2 * rows
    head = wout.shape[0]
    units = wup.shape[1]
    tile = min(512, dim)
    utile = min(512, units)
    wide = min(2048, dim)

    me = lax.axis_index("tp")
    core = lax.rem(me, 2)
    chip = me // 2
    right, left = lax.rem(me + 2, n), lax.rem(me + n - 2, n)
    sibling = me + 1 - 2 * core
    target = (right, left)
    crossed = (right + 1 - 2 * core, left + 1 - 2 * core)

    def slot_of(offset):
        if offset == 0:
            return 0
        if abs(offset) == far:
            return 1
        return 2 * abs(offset) + (1 if offset > 0 else 0)

    def slot_chip(slot):
        if slot == 0:
            return chip
        if slot == 1:
            return lax.rem(chip + far, chips)
        offset = slot // 2 if slot % 2 else -(slot // 2)
        return lax.rem(chip + chips + offset, chips)

    def signed(direction, distance):
        return -distance if direction == RIGHT else distance

    def quarter_rows(which, t):
        return pl.ds(which * half_rows + t * quarter, quarter)

    def half_ds(which):
        return pl.ds(which * half_rows, half_rows)

    def messages(direction):
        a, b = direction, 1 - direction
        out = [(0, a, 0), (0, b, 0), (0, a, 1), (0, b, 1)]
        for j in range(1, far - 1):
            out += [(j, a, 0), (j, a, 1), (j, b, 0), (j, b, 1)]
        return out + [(far - 1, a, 0), (far - 1, a, 1)]

    plans = (messages(RIGHT), messages(LEFT))
    count = len(plans[0])

    def width_of(which, t, with_ids):
        return dim + ID_COLS if with_ids and which == 0 and t == 0 else dim

    def ag_ref(direction, m, extra, with_ids):
        j, which, t = plans[direction][m]
        return hbuf.at[slot_of(signed(direction, j + extra)), core, quarter_rows(which, t), pl.ds(0, width_of(which, t, with_ids))]

    def ag_copy(direction, m, with_ids):
        return pltpu.make_async_remote_copy(
            src_ref=ag_ref(direction, m, 0, with_ids), dst_ref=ag_ref(direction, m, 1, with_ids),
            send_sem=ag_send.at[direction, m], recv_sem=ag_recv.at[direction, m],
            device_id={"tp": target[direction]}, device_id_type=MESH)

    def sib_copy(direction, m, with_ids):
        ref = ag_ref(direction, m, 1, with_ids)
        return pltpu.make_async_remote_copy(
            src_ref=ref, dst_ref=ref, send_sem=sib_send.at[direction, m], recv_sem=sib_recv.at[direction, m],
            device_id={"tp": sibling}, device_id_type=MESH)

    def own_copy(which, t, with_ids):
        ref = hbuf.at[0, core, quarter_rows(which, t), pl.ds(0, width_of(which, t, with_ids))]
        return pltpu.make_async_remote_copy(
            src_ref=ref, dst_ref=ref, send_sem=own_send.at[which, t], recv_sem=own_recv.at[which, t],
            device_id={"tp": sibling}, device_id_type=MESH)

    def part_copy(slot, which, t):
        rws = quarter_rows(which, t)
        return pltpu.make_async_remote_copy(
            src_ref=part.at[slot, 1 - core, rws], dst_ref=psib.at[slot, rws],
            send_sem=part_send.at[slot, which, t], recv_sem=part_recv.at[slot, which, t],
            device_id={"tp": sibling}, device_id_type=MESH)

    def rs_plan(direction, m):
        if m == steps - 1:
            which, distance, before = 0, 1, m - 1
        elif m % 2 == 0:
            which, distance, before = 1, far - 1 - m // 2, m - 2
        else:
            which, distance, before = 0, far - m // 2, m - 2
        dest = slot_of(-signed(direction, distance))
        return which ^ direction, dest, (before if m >= 2 else None)

    def rs_copy(direction, m, t):
        before = rs_plan(direction, m)[2]
        src = fresh.at[direction, t] if before is None else ring.at[direction, before, t]
        return pltpu.make_async_remote_copy(
            src_ref=src, dst_ref=ring.at[direction, m, t], send_sem=rs_send.at[direction, m, t], recv_sem=rs_recv.at[direction, m, t],
            device_id={"tp": target[direction]}, device_id_type=MESH)

    def lead_copy(direction, t, cross):
        which, dest, _ = rs_plan(direction, 0)
        return pltpu.make_async_remote_copy(
            src_ref=part.at[dest, 1 - core if cross else core, quarter_rows(which, t)], dst_ref=lead.at[direction, t, cross],
            send_sem=lead_send.at[direction, t, cross], recv_sem=lead_recv.at[direction, t, cross],
            device_id={"tp": (crossed if cross else target)[direction]}, device_id_type=MESH)

    def lead_send_all(t):
        for cross in (0, 1):
            for direction in (RIGHT, LEFT):
                lead_copy(direction, t, cross).start()

    def sum_send(m, t, need):
        for direction in (RIGHT, LEFT):
            which, dest, before = rs_plan(direction, m)
            need(dest, which, t)
            if before == 0:
                for cross in (0, 1):
                    lead_copy(direction, t, cross).wait_recv()
            elif before is not None:
                rs_copy(direction, before, t).wait_recv()
            rws = quarter_rows(which, t)

            def add(i):
                cs = cols_at(i, tile)
                total = part[dest, core, rws, cs].astype(F32) + psib[dest, rws, cs].astype(F32)
                if before is None:
                    fresh[direction, t, :, cs] = total
                elif before == 0:
                    first = lead[direction, t, 0, :, cs].astype(F32) + lead[direction, t, 1, :, cs].astype(F32)
                    ring[direction, 0, t, :, cs] = first + total
                else:
                    ring[direction, before, t, :, cs] = ring[direction, before, t, :, cs] + total

            loop(dim // tile, add)
            rs_copy(direction, m, t).start()

    def rs_step(m, need):
        for t in range(2):
            sum_send(m, t, need)

    def weight_copy(src, dst, index):
        return pltpu.make_async_copy(src, dst, w_sem.at[index])

    def norm_send(t, sums, layer, gain_ref, shift_ref, with_ids, before_send=None):
        means = [jnp.sum(s, axis=1, keepdims=True) / dim for s in sums]

        def sq_body(i, acc):
            out = []
            for which in range(2):
                centered = resid[quarter_rows(which, t), cols_at(i, tile)] - means[which]
                out.append(acc[which] + centered * centered)
            return tuple(out)

        zero = jnp.zeros((quarter, tile), F32)
        squares = lax.fori_loop(0, dim // tile, sq_body, (zero, zero))
        scales = [lax.rsqrt(jnp.sum(s, axis=1, keepdims=True) / dim + 1e-5) for s in squares]

        def out_body(i):
            cs = cols_at(i, tile)
            for which in range(2):
                rws = quarter_rows(which, t)
                value = (resid[rws, cs] - means[which]) * scales[which] * gain_ref[pl.ds(layer, 1), cs] + shift_ref[pl.ds(layer, 1), cs]
                hbuf[0, core, rws, cs] = value.astype(BF16)

        loop(dim // tile, out_body)
        if before_send is not None:
            before_send()
        for i in range(2):
            for direction in (RIGHT, LEFT):
                ag_copy(direction, 2 * t + i, with_ids).start()
        for which in range(2):
            own_copy(which, t, with_ids).start()

    def finish(t, layer, bias_ref):
        for which in range(2):
            rs_copy(1 - which, steps - 3, t).wait_recv()
            rs_copy(which, steps - 1, t).wait_recv()

        def body(i, acc):
            cs = cols_at(i, tile)
            out = []
            for which in range(2):
                rws = quarter_rows(which, t)
                total = part[0, core, rws, cs].astype(F32) + psib[0, rws, cs].astype(F32)
                total = total + ring[1 - which, steps - 3, t, :, cs] + ring[which, steps - 1, t, :, cs]
                value = resid[rws, cs] + (total + bias_ref[pl.ds(layer, 1), cs])
                resid[rws, cs] = value
                out_ref[rws, cs] = value.astype(BF16)
                out.append(acc[which] + value)
            return tuple(out)

        zero = jnp.zeros((quarter, tile), F32)
        return lax.fori_loop(0, dim // tile, body, (zero, zero))

    def boundary(layer, bias_ref, next_layer, gain_ref, shift_ref, with_ids, more=None):
        for t in range(2):
            sums = finish(t, layer, bias_ref)
            if more is None:
                norm_send(t, sums, next_layer, gain_ref, shift_ref, with_ids)
            else:
                @pl.when(more)
                def _():
                    norm_send(t, sums, next_layer, gain_ref, shift_ref, with_ids)
        for direction in (RIGHT, LEFT):
            for t in range(2):
                for cross in (0, 1):
                    lead_copy(direction, t, cross).wait_send()
                for m in range(1, steps):
                    rs_copy(direction, m, t).wait_send()
        for piece in exchanged:
            part_copy(*piece).wait_send()

    def needs():
        seen = set()

        def need(*piece):
            if piece not in seen:
                seen.add(piece)
                part_copy(*piece).wait_recv()

        return need

    def need_all(need):
        for piece in exchanged:
            need(*piece)

    def gather_step(m, with_ids):
        for direction in (RIGHT, LEFT):
            ag_copy(direction, m, with_ids).wait_recv()
            j, which, t = plans[direction][m]
            if (j + 1, which, t) in plans[direction]:
                ag_copy(direction, plans[direction].index((j + 1, which, t)), with_ids).start()
            sib_copy(direction, m, with_ids).start()

    def sib_wait(first, last, with_ids):
        for m in range(first, last + 1):
            for direction in (RIGHT, LEFT):
                sib_copy(direction, m, with_ids).wait_recv()

    def own_wait(with_ids):
        for which in range(2):
            for t in range(2):
                own_copy(which, t, with_ids).wait_recv()

    def gather_end(with_ids):
        for which in range(2):
            for t in range(2):
                own_copy(which, t, with_ids).wait_send()
        for m in range(count):
            for direction in (RIGHT, LEFT):
                ag_copy(direction, m, with_ids).wait_send()
                sib_copy(direction, m, with_ids).wait_send()

    def piece_rows(piece):
        slot, which, t = piece
        return half_ds(which) if t is None else quarter_rows(which, t)

    def piece_size(piece):
        return rows if piece[2] is None else half_rows

    def load_rows(pieces):
        return jnp.concatenate([hbuf[p[0], :, piece_rows(p), pl.ds(0, dim)].reshape(piece_size(p), dim) for p in pieces], axis=0)

    def store_part(pieces, value, cs):
        start = 0
        for p in pieces:
            size = piece_size(p)
            part[p[0], :, piece_rows(p), cs] = value[start:start + size].reshape(2, size // 2, value.shape[1])
            start += size

    def both(slot):
        return [(slot, 0, None), (slot, 1, None)]

    minus, plus = slot_of(-(far - 1)), slot_of(far - 1)
    own = both(0)
    farthest = both(1)
    leading = [(minus, 0, None), (plus, 1, None)]
    trailing = [(minus, 1, None), (plus, 0, None)]

    exchanged = [(slot, which, t) for slot in range(chips) for which in range(2) for t in range(2) if (slot, which, None) not in leading]

    def near(p):
        return both(2 * p) + both(2 * p + 1)

    lead_at = 4 * (far - 2) + 1
    last_at = count - 1

    def send_parts(pieces):
        for slot, which, t in pieces:
            for u in range(2) if t is None else (t,):
                part_copy(slot, which, u).start()

    def attention_half(layer):
        need = needs()

        def project(pieces, kinds=(0, 3)):
            def body(t):
                value = jnp.dot(load_rows(pieces), wqkv[t], preferred_element_type=F32).astype(BF16)
                start = 0
                for p in pieces:
                    size = piece_size(p)
                    qkv[t, p[0], :, piece_rows(p)] = value[start:start + size].reshape(2, size // 2, head)
                    start += size

            lax.fori_loop(kinds[0], kinds[1], lambda t, carry: (body(t), carry)[1], 0)

        def slot_ids(slot):
            cs = pl.ds(slot * chip_rows, chip_rows)
            lines = [hbuf[slot, c, pl.ds(0, 8), pl.ds(dim, ID_COLS)].astype(F32)[:, 0:rows] for c in range(2)]
            kids[:, cs] = jnp.concatenate(lines, axis=1)

        def column_ids(piece):
            line = kids[0:1, pl.ds(piece[0] * chip_rows, chip_rows)]
            column = jnp.broadcast_to(line, (chip_rows, chip_rows)).T[:, 0:1]
            size = piece_size(piece) // 2
            first = piece[1] * half_rows + (piece[2] or 0) * quarter
            return jnp.concatenate([column[c * rows + first:c * rows + first + size] for c in range(2)], axis=0)

        def column_pos(piece):
            size = piece_size(piece) // 2
            first = piece[1] * half_rows + (piece[2] or 0) * quarter
            i = lax.broadcasted_iota(jnp.int32, (2 * size, 1), 0)
            i = i + jnp.where(i >= size, rows - size, 0)
            return i + (first + slot_chip(piece[0]) * chip_rows)

        def attend(pieces):
            keys = qkv[1].reshape(chips * chip_rows, head)
            values = qkv[2].reshape(chips * chip_rows, head)
            queries = jnp.concatenate([qkv[0, p[0], :, piece_rows(p)].reshape(piece_size(p), head) for p in pieces], axis=0)
            scores = lax.dot_general(queries, keys, (((1,), (1,)), ((), ())), preferred_element_type=F32) * (head ** -0.5)
            ids_col = jnp.concatenate([column_ids(piece) for piece in pieces], axis=0)
            pos_col = jnp.concatenate([column_pos(piece) for piece in pieces], axis=0)
            allowed = (kpos[0:1, :] <= pos_col) & (kids[0:1, :] == ids_col)
            scores = jnp.where(allowed, scores, -1e30)
            top = jnp.max(scores, axis=1, keepdims=True)
            probs = jnp.exp(scores - top)
            probs = (probs * (1.0 / jnp.sum(probs, axis=1, keepdims=True))).astype(BF16)
            mixed = jnp.dot(probs, values, preferred_element_type=F32).astype(BF16)

            def proj(c):
                cs = cols_at(c, wide)
                store_part(pieces, jnp.dot(mixed, wout[:, cs], preferred_element_type=F32).astype(BF16), cs)

            loop(dim // wide, proj)

        weight_copy(wup_hbm.at[layer], wup, 2).start()
        weight_copy(wdown_hbm.at[layer], wdown, 3).start()
        weight_copy(wqkv_hbm.at[layer], wqkv, 0).wait()
        weight_copy(wout_hbm.at[layer], wout, 1).wait()
        for m in range(count):
            gather_step(m, True)
            if m == 0:
                own_wait(True)
                project(own)
                slot_ids(0)
            for p in range(1, far - 1):
                if m == 4 * p:
                    sib_wait(4 * p - 4, 4 * p - 1, True)
                    project(near(p))
                    slot_ids(2 * p)
                    slot_ids(2 * p + 1)
            if m == last_at - 2:
                sib_wait(lead_at - 1, m, True)
                project(leading + trailing)
                slot_ids(minus)
                slot_ids(plus)
            if m >= last_at - 1:
                t = m - last_at + 1
                sib_wait(m, m, True)
                project([(slot, which, t) for slot, which, _ in farthest], (1, 3))
                if t == 0:
                    slot_ids(1)
        for t in range(2):
            quarters = [(slot, which, t) for slot, which, _ in leading]
            attend(quarters)
            lead_send_all(t)
        project(farthest, (0, 1))
        attend(farthest)
        send_parts(farthest)
        rs_step(1, need)
        gather_end(True)
        attend(trailing)
        send_parts(trailing)
        for p in range(far - 2, 0, -1):
            for pieces in (both(2 * p), both(2 * p + 1)) + ((own,) if p == 1 else ()):
                attend(pieces)
                send_parts(pieces)
            rs_step(2 * (far - 1 - p), need)
            rs_step(2 * (far - 1 - p) + 1, need)
        rs_step(steps - 1, need)
        need_all(need)

    def mlp_half(layer):
        need = needs()

        def up(pieces):
            count_rows = rows * len(pieces)

            def body(c):
                cs = cols_at(c, utile)
                x = jnp.dot(load_rows(pieces), wup[:, cs], preferred_element_type=F32) + ub_ref[pl.ds(layer, 1), cs]
                inner = 0.7978845608028654 * (x + 0.044715 * (x * x * x))
                hidden[pl.ds(0, count_rows), cs] = (0.5 * x * (1.0 + jnp.tanh(inner))).astype(BF16)

            loop(units // utile, body)

        def down(pieces):
            count_rows = rows * len(pieces)
            step = min(wide, dim * 2 * rows // (2 * count_rows))

            def body(c):
                cs = cols_at(c, step)
                value = jnp.dot(hidden[pl.ds(0, count_rows), :], wdown[:, cs], preferred_element_type=F32).astype(BF16)
                store_part(pieces, value, cs)

            loop(dim // step, body)

        weight_copy(wup_hbm.at[layer], wup, 2).wait()
        weight_copy(wdown_hbm.at[layer], wdown, 3).wait()

        @pl.when(layer + 1 < layers)
        def _():
            weight_copy(wqkv_hbm.at[layer + 1], wqkv, 0).start()
            weight_copy(wout_hbm.at[layer + 1], wout, 1).start()

        for m in range(last_at):
            gather_step(m, False)
            if m == 0:
                own_wait(False)
                up(own)
            if m == 1:
                down(own)
                send_parts(own)
            for p in range(1, far - 2):
                if m == 4 * p:
                    sib_wait(4 * p - 4, 4 * p - 1, False)
                    up(near(p))
                if m == 4 * p + 1:
                    down(near(p))
                    send_parts(near(p))
            if m == lead_at:
                sib_wait(lead_at - 5, lead_at, False)
                up(leading)
                down(leading)
                for t in range(2):
                    lead_send_all(t)
        gather_step(last_at, False)
        sib_wait(lead_at + 1, last_at, False)
        up(farthest + trailing)
        down(farthest + trailing)
        send_parts(farthest + trailing)
        rs_step(1, need)
        gather_end(False)
        up(near(far - 2))
        down(near(far - 2))
        send_parts(near(far - 2))
        for m in range(2, steps):
            rs_step(m, need)
        need_all(need)

    weight_copy(wqkv_hbm.at[0], wqkv, 0).start()
    weight_copy(wout_hbm.at[0], wout, 1).start()
    barrier = pltpu.get_barrier_semaphore()
    for device in (left, right, sibling) + crossed:
        pl.semaphore_signal(barrier, inc=1, device_id={"tp": device}, device_id_type=MESH)
    hbuf[0, core, pl.ds(0, quarter), pl.ds(dim, ID_COLS)] = jnp.zeros((quarter, ID_COLS), BF16)
    hbuf[0, core, pl.ds(0, quarter), pl.ds(dim, rows)] = jnp.broadcast_to(ids_ref[...].astype(F32).astype(BF16), (quarter, rows))
    for slot in range(chips):
        kpos[:, pl.ds(slot * chip_rows, chip_rows)] = lax.broadcasted_iota(jnp.int32, (8, chip_rows), 1) + slot_chip(slot) * chip_rows
    for t in range(2):
        def widen(i, acc):
            out = []
            for which in range(2):
                rws = quarter_rows(which, t)
                value = tokens_ref[rws, cols_at(i, tile)].astype(F32)
                resid[rws, cols_at(i, tile)] = value
                out.append(acc[which] + value)
            return tuple(out)

        zero = jnp.zeros((quarter, tile), F32)
        sums = lax.fori_loop(0, dim // tile, widen, (zero, zero))
        norm_send(t, sums, 0, g1_ref, s1_ref, True, (lambda: pl.semaphore_wait(barrier, 5)) if t == 0 else None)

    def layer_body(layer):
        attention_half(layer)
        boundary(layer, ob_ref, layer, g2_ref, s2_ref, False)
        mlp_half(layer)
        boundary(layer, db_ref, lax.rem(layer + 1, layers), g1_ref, s1_ref, True, layer + 1 < layers)

    loop(layers, layer_body)


def solution(mesh):
    n = mesh.shape["tp"]
    chips = n // 2
    far = chips // 2
    steps = 2 * far - 1
    sends = 4 * far - 2
    row_spec = P("dp", "tp", None)
    vec_spec = P(None, None)
    in_specs = (row_spec, P("dp", "tp"), vec_spec, vec_spec, P(None, None, None, "tp", None), P(None, "tp", None, None), vec_spec, vec_spec, vec_spec, P(None, None, "tp"), P(None, "tp"), P(None, "tp", None), vec_spec)

    def device_fn(tokens, doc_ids, norm1_gain, norm1_shift, qkv_weight, out_weight, out_bias, norm2_gain, norm2_shift, up_weight, up_bias, down_weight, down_bias):
        batch, rows, dim = tokens.shape
        layers = norm1_gain.shape[0]
        head = qkv_weight.shape[-1]
        units = up_weight.shape[-1]
        wqkv = jnp.transpose(qkv_weight, (0, 2, 3, 1, 4)).reshape(layers, 3, dim, head)
        wout = out_weight.reshape(layers, head, dim)
        vmem = pl.BlockSpec(memory_space=pltpu.VMEM)
        hbm = pl.BlockSpec(memory_space=pl.ANY)
        dma = pltpu.SemaphoreType.DMA
        result = pl.pallas_call(
            functools.partial(block_kernel, n),
            out_shape=jax.ShapeDtypeStruct((rows, dim), BF16),
            in_specs=[vmem] * 9 + [hbm] * 4,
            out_specs=vmem,
            scratch_shapes=[
                pltpu.VMEM((chips, 2, rows, dim + ID_COLS), BF16),
                pltpu.VMEM((chips, 2, rows, dim), BF16),
                pltpu.VMEM((chips, rows, dim), BF16),
                pltpu.VMEM((2, steps, 2, rows // 4, dim), F32),
                pltpu.VMEM((2, 2, rows // 4, dim), F32),
                pltpu.VMEM((2, 2, 2, rows // 4, dim), BF16),
                pltpu.VMEM((rows, dim), F32),
                pltpu.VMEM((3, dim, head), BF16),
                pltpu.VMEM((head, dim), BF16),
                pltpu.VMEM((dim, units), BF16),
                pltpu.VMEM((units, dim), BF16),
                pltpu.VMEM((3, chips, 2, rows, head), BF16),
                pltpu.VMEM((4 * rows, units), BF16),
                pltpu.VMEM((8, chips * 2 * rows), jnp.int32),
                pltpu.VMEM((8, chips * 2 * rows), F32),
                dma((2, sends)), dma((2, sends)), dma((2, sends)), dma((2, sends)), dma((2, 2)), dma((2, 2)),
                dma((chips, 2, 2)), dma((chips, 2, 2)), dma((2, steps, 2)), dma((2, steps, 2)), dma((2, 2, 2)), dma((2, 2, 2)), dma((4,)),
            ],
            compiler_params=pltpu.CompilerParams(collective_id=0, has_side_effects=True, vmem_limit_bytes=67043328),
        )(tokens.reshape(rows, dim), doc_ids, norm1_gain, norm1_shift, out_bias, norm2_gain, norm2_shift, up_bias, down_bias, wqkv, wout, up_weight, down_weight)
        return result.reshape(batch, rows, dim)

    return jax.shard_map(device_fn, mesh=mesh, in_specs=in_specs, out_specs=row_spec, check_vma=False)
```

```python
import functools

import jax
import jax.numpy as jnp
from jax import lax
from jax.experimental import pallas as pl
from jax.experimental.pallas import tpu as pltpu
from jax.sharding import PartitionSpec as P

MESH = pl.DeviceIdType.MESH
F32, BF16 = jnp.float32, jnp.bfloat16
ID_COLS = 128
RIGHT, LEFT = 0, 1


def loop(count, body):
    lax.fori_loop(0, count, lambda i, carry: (body(i), carry)[1], 0)


def cols_at(i, width):
    return pl.ds(pl.multiple_of(i * width, width), width)


def block_kernel(n, tokens_ref, ids_ref, g1_ref, s1_ref, ob_ref, g2_ref, s2_ref, ub_ref, db_ref, wqkv_hbm, wout_hbm, wup_hbm, wdown_hbm,
                 out_ref, hbuf, part, psib, ring, fresh, lead, resid, wqkv, wout, wup, wdown, qkv, hidden, kpos, kids,
                 ag_send, ag_recv, sib_send, sib_recv, own_send, own_recv, part_send, part_recv, rs_send, rs_recv, lead_send, lead_recv, w_sem):
    chips = n // 2
    far = chips // 2
    steps = 2 * far - 1
    layers = g1_ref.shape[0]
    rows, dim = tokens_ref.shape
    half_rows, quarter = rows // 2, rows // 4
    chip_rows = 2 * rows
    head = wout.shape[0]
    units = wup.shape[1]
    tile = min(512, dim)
    utile = min(512, units)
    wide = min(2048, dim)

    me = lax.axis_index("tp")
    core = lax.rem(me, 2)
    chip = me // 2
    right, left = lax.rem(me + 2, n), lax.rem(me + n - 2, n)
    sibling = me + 1 - 2 * core
    target = (right, left)
    crossed = (right + 1 - 2 * core, left + 1 - 2 * core)

    def slot_of(offset):
        if offset == 0:
            return 0
        if abs(offset) == far:
            return 1
        return 2 * abs(offset) + (1 if offset > 0 else 0)

    def slot_chip(slot):
        if slot == 0:
            return chip
        if slot == 1:
            return lax.rem(chip + far, chips)
        offset = slot // 2 if slot % 2 else -(slot // 2)
        return lax.rem(chip + chips + offset, chips)

    def signed(direction, distance):
        return -distance if direction == RIGHT else distance

    def quarter_rows(which, t):
        return pl.ds(which * half_rows + t * quarter, quarter)

    def half_ds(which):
        return pl.ds(which * half_rows, half_rows)

    def messages(direction):
        a, b = direction, 1 - direction
        out = [(0, a, 0), (0, b, 0), (0, a, 1), (0, b, 1)]
        for j in range(1, far - 1):
            out += [(j, a, 0), (j, a, 1), (j, b, 0), (j, b, 1)]
        return out + [(far - 1, a, 0), (far - 1, a, 1)]

    plans = (messages(RIGHT), messages(LEFT))
    count = len(plans[0])

    def width_of(which, t, with_ids):
        return dim + ID_COLS if with_ids and which == 0 and t == 0 else dim

    def ag_ref(direction, m, extra, with_ids):
        j, which, t = plans[direction][m]
        return hbuf.at[slot_of(signed(direction, j + extra)), core, quarter_rows(which, t), pl.ds(0, width_of(which, t, with_ids))]

    def ag_copy(direction, m, with_ids):
        return pltpu.make_async_remote_copy(
            src_ref=ag_ref(direction, m, 0, with_ids), dst_ref=ag_ref(direction, m, 1, with_ids),
            send_sem=ag_send.at[direction, m], recv_sem=ag_recv.at[direction, m],
            device_id={"tp": target[direction]}, device_id_type=MESH)

    def sib_copy(direction, m, with_ids):
        ref = ag_ref(direction, m, 1, with_ids)
        return pltpu.make_async_remote_copy(
            src_ref=ref, dst_ref=ref, send_sem=sib_send.at[direction, m], recv_sem=sib_recv.at[direction, m],
            device_id={"tp": sibling}, device_id_type=MESH)

    def own_copy(which, t, with_ids):
        ref = hbuf.at[0, core, quarter_rows(which, t), pl.ds(0, width_of(which, t, with_ids))]
        return pltpu.make_async_remote_copy(
            src_ref=ref, dst_ref=ref, send_sem=own_send.at[which, t], recv_sem=own_recv.at[which, t],
            device_id={"tp": sibling}, device_id_type=MESH)

    def part_copy(slot, which, t):
        rws = quarter_rows(which, t)
        return pltpu.make_async_remote_copy(
            src_ref=part.at[slot, 1 - core, rws], dst_ref=psib.at[slot, rws],
            send_sem=part_send.at[slot, which, t], recv_sem=part_recv.at[slot, which, t],
            device_id={"tp": sibling}, device_id_type=MESH)

    def rs_plan(direction, m):
        if m == steps - 1:
            which, distance, before = 0, 1, m - 1
        elif m % 2 == 0:
            which, distance, before = 1, far - 1 - m // 2, m - 2
        else:
            which, distance, before = 0, far - m // 2, m - 2
        dest = slot_of(-signed(direction, distance))
        return which ^ direction, dest, (before if m >= 2 else None)

    def rs_copy(direction, m, t):
        before = rs_plan(direction, m)[2]
        src = fresh.at[direction, t] if before is None else ring.at[direction, before, t]
        return pltpu.make_async_remote_copy(
            src_ref=src, dst_ref=ring.at[direction, m, t], send_sem=rs_send.at[direction, m, t], recv_sem=rs_recv.at[direction, m, t],
            device_id={"tp": target[direction]}, device_id_type=MESH)

    def lead_copy(direction, t, cross):
        which, dest, _ = rs_plan(direction, 0)
        return pltpu.make_async_remote_copy(
            src_ref=part.at[dest, 1 - core if cross else core, quarter_rows(which, t)], dst_ref=lead.at[direction, t, cross],
            send_sem=lead_send.at[direction, t, cross], recv_sem=lead_recv.at[direction, t, cross],
            device_id={"tp": (crossed if cross else target)[direction]}, device_id_type=MESH)

    def lead_send_all(t):
        for cross in (0, 1):
            for direction in (RIGHT, LEFT):
                lead_copy(direction, t, cross).start()

    def sum_send(m, t, need):
        for direction in (RIGHT, LEFT):
            which, dest, before = rs_plan(direction, m)
            need(dest, which, t)
            if before == 0:
                for cross in (0, 1):
                    lead_copy(direction, t, cross).wait_recv()
            elif before is not None:
                rs_copy(direction, before, t).wait_recv()
            rws = quarter_rows(which, t)

            def add(i):
                cs = cols_at(i, tile)
                total = part[dest, core, rws, cs].astype(F32) + psib[dest, rws, cs].astype(F32)
                if before is None:
                    fresh[direction, t, :, cs] = total
                elif before == 0:
                    first = lead[direction, t, 0, :, cs].astype(F32) + lead[direction, t, 1, :, cs].astype(F32)
                    ring[direction, 0, t, :, cs] = first + total
                else:
                    ring[direction, before, t, :, cs] = ring[direction, before, t, :, cs] + total

            loop(dim // tile, add)
            rs_copy(direction, m, t).start()

    def rs_step(m, need):
        for t in range(2):
            sum_send(m, t, need)

    def weight_copy(src, dst, index):
        return pltpu.make_async_copy(src, dst, w_sem.at[index])

    def norm_send(t, sums, layer, gain_ref, shift_ref, with_ids, before_send=None):
        means = [jnp.sum(s, axis=1, keepdims=True) / dim for s in sums]

        def sq_body(i, acc):
            out = []
            for which in range(2):
                centered = resid[quarter_rows(which, t), cols_at(i, tile)] - means[which]
                out.append(acc[which] + centered * centered)
            return tuple(out)

        zero = jnp.zeros((quarter, tile), F32)
        squares = lax.fori_loop(0, dim // tile, sq_body, (zero, zero))
        scales = [lax.rsqrt(jnp.sum(s, axis=1, keepdims=True) / dim + 1e-5) for s in squares]

        def out_body(i):
            cs = cols_at(i, tile)
            for which in range(2):
                rws = quarter_rows(which, t)
                value = (resid[rws, cs] - means[which]) * scales[which] * gain_ref[pl.ds(layer, 1), cs] + shift_ref[pl.ds(layer, 1), cs]
                hbuf[0, core, rws, cs] = value.astype(BF16)

        loop(dim // tile, out_body)
        if before_send is not None:
            before_send()
        for i in range(2):
            for direction in (RIGHT, LEFT):
                ag_copy(direction, 2 * t + i, with_ids).start()
        for which in range(2):
            own_copy(which, t, with_ids).start()

    def finish(t, layer, bias_ref):
        for which in range(2):
            rs_copy(1 - which, steps - 3, t).wait_recv()
            rs_copy(which, steps - 1, t).wait_recv()

        def body(i, acc):
            cs = cols_at(i, tile)
            out = []
            for which in range(2):
                rws = quarter_rows(which, t)
                total = part[0, core, rws, cs].astype(F32) + psib[0, rws, cs].astype(F32)
                total = total + ring[1 - which, steps - 3, t, :, cs] + ring[which, steps - 1, t, :, cs]
                value = resid[rws, cs] + (total + bias_ref[pl.ds(layer, 1), cs])
                resid[rws, cs] = value
                out_ref[rws, cs] = value.astype(BF16)
                out.append(acc[which] + value)
            return tuple(out)

        zero = jnp.zeros((quarter, tile), F32)
        return lax.fori_loop(0, dim // tile, body, (zero, zero))

    def boundary(layer, bias_ref, next_layer, gain_ref, shift_ref, with_ids, more=None):
        for t in range(2):
            sums = finish(t, layer, bias_ref)
            if more is None:
                norm_send(t, sums, next_layer, gain_ref, shift_ref, with_ids)
            else:
                @pl.when(more)
                def _():
                    norm_send(t, sums, next_layer, gain_ref, shift_ref, with_ids)
        for direction in (RIGHT, LEFT):
            for t in range(2):
                for cross in (0, 1):
                    lead_copy(direction, t, cross).wait_send()
                for m in range(1, steps):
                    rs_copy(direction, m, t).wait_send()
        for piece in exchanged:
            part_copy(*piece).wait_send()

    def needs():
        seen = set()

        def need(*piece):
            if piece not in seen:
                seen.add(piece)
                part_copy(*piece).wait_recv()

        return need

    def need_all(need):
        for piece in exchanged:
            need(*piece)

    def gather_step(m, with_ids):
        for direction in (RIGHT, LEFT):
            ag_copy(direction, m, with_ids).wait_recv()
            j, which, t = plans[direction][m]
            if (j + 1, which, t) in plans[direction]:
                ag_copy(direction, plans[direction].index((j + 1, which, t)), with_ids).start()
            sib_copy(direction, m, with_ids).start()

    def sib_wait(first, last, with_ids):
        for m in range(first, last + 1):
            for direction in (RIGHT, LEFT):
                sib_copy(direction, m, with_ids).wait_recv()

    def own_wait(with_ids):
        for which in range(2):
            for t in range(2):
                own_copy(which, t, with_ids).wait_recv()

    def gather_end(with_ids):
        for which in range(2):
            for t in range(2):
                own_copy(which, t, with_ids).wait_send()
        for m in range(count):
            for direction in (RIGHT, LEFT):
                ag_copy(direction, m, with_ids).wait_send()
                sib_copy(direction, m, with_ids).wait_send()

    def piece_rows(piece):
        slot, which, t = piece
        return half_ds(which) if t is None else quarter_rows(which, t)

    def piece_size(piece):
        return rows if piece[2] is None else half_rows

    def load_rows(pieces):
        return jnp.concatenate([hbuf[p[0], :, piece_rows(p), pl.ds(0, dim)].reshape(piece_size(p), dim) for p in pieces], axis=0)

    def store_part(pieces, value, cs):
        start = 0
        for p in pieces:
            size = piece_size(p)
            part[p[0], :, piece_rows(p), cs] = value[start:start + size].reshape(2, size // 2, value.shape[1])
            start += size

    def both(slot):
        return [(slot, 0, None), (slot, 1, None)]

    minus, plus = slot_of(-(far - 1)), slot_of(far - 1)
    own = both(0)
    farthest = both(1)
    leading = [(minus, 0, None), (plus, 1, None)]
    trailing = [(minus, 1, None), (plus, 0, None)]

    exchanged = [(slot, which, t) for slot in range(chips) for which in range(2) for t in range(2) if (slot, which, None) not in leading]

    def near(p):
        return both(2 * p) + both(2 * p + 1)

    lead_at = 4 * (far - 2) + 1
    last_at = count - 1

    def send_parts(pieces):
        for slot, which, t in pieces:
            for u in range(2) if t is None else (t,):
                part_copy(slot, which, u).start()

    def attention_half(layer):
        need = needs()

        def project(pieces, kinds=(0, 3)):
            def body(t):
                value = jnp.dot(load_rows(pieces), wqkv[t], preferred_element_type=F32).astype(BF16)
                start = 0
                for p in pieces:
                    size = piece_size(p)
                    qkv[t, p[0], :, piece_rows(p)] = value[start:start + size].reshape(2, size // 2, head)
                    start += size

            lax.fori_loop(kinds[0], kinds[1], lambda t, carry: (body(t), carry)[1], 0)

        def slot_ids(slot):
            cs = pl.ds(slot * chip_rows, chip_rows)
            lines = [hbuf[slot, c, pl.ds(0, 8), pl.ds(dim, ID_COLS)].astype(F32)[:, 0:rows] for c in range(2)]
            kids[:, cs] = jnp.concatenate(lines, axis=1)

        def column_ids(piece):
            line = kids[0:1, pl.ds(piece[0] * chip_rows, chip_rows)]
            column = jnp.broadcast_to(line, (chip_rows, chip_rows)).T[:, 0:1]
            size = piece_size(piece) // 2
            first = piece[1] * half_rows + (piece[2] or 0) * quarter
            return jnp.concatenate([column[c * rows + first:c * rows + first + size] for c in range(2)], axis=0)

        def column_pos(piece):
            size = piece_size(piece) // 2
            first = piece[1] * half_rows + (piece[2] or 0) * quarter
            i = lax.broadcasted_iota(jnp.int32, (2 * size, 1), 0)
            i = i + jnp.where(i >= size, rows - size, 0)
            return i + (first + slot_chip(piece[0]) * chip_rows)

        def attend(pieces):
            keys = qkv[1].reshape(chips * chip_rows, head)
            values = qkv[2].reshape(chips * chip_rows, head)
            queries = jnp.concatenate([qkv[0, p[0], :, piece_rows(p)].reshape(piece_size(p), head) for p in pieces], axis=0)
            scores = lax.dot_general(queries, keys, (((1,), (1,)), ((), ())), preferred_element_type=F32) * (head ** -0.5)
            ids_col = jnp.concatenate([column_ids(piece) for piece in pieces], axis=0)
            pos_col = jnp.concatenate([column_pos(piece) for piece in pieces], axis=0)
            allowed = (kpos[0:1, :] <= pos_col) & (kids[0:1, :] == ids_col)
            scores = jnp.where(allowed, scores, -1e30)
            top = jnp.max(scores, axis=1, keepdims=True)
            probs = jnp.exp(scores - top)
            probs = (probs * (1.0 / jnp.sum(probs, axis=1, keepdims=True))).astype(BF16)
            mixed = jnp.dot(probs, values, preferred_element_type=F32).astype(BF16)

            def proj(c):
                cs = cols_at(c, wide)
                store_part(pieces, jnp.dot(mixed, wout[:, cs], preferred_element_type=F32).astype(BF16), cs)

            loop(dim // wide, proj)

        weight_copy(wup_hbm.at[layer], wup, 2).start()
        weight_copy(wdown_hbm.at[layer], wdown, 3).start()
        weight_copy(wqkv_hbm.at[layer], wqkv, 0).wait()
        weight_copy(wout_hbm.at[layer], wout, 1).wait()
        for m in range(count):
            gather_step(m, True)
            if m == 0:
                own_wait(True)
                project(own)
                slot_ids(0)
            for p in range(1, far - 1):
                if m == 4 * p:
                    sib_wait(4 * p - 4, 4 * p - 1, True)
                    project(near(p))
                    slot_ids(2 * p)
                    slot_ids(2 * p + 1)
            if m == last_at - 2:
                sib_wait(lead_at - 1, m, True)
                project(leading + trailing)
                slot_ids(minus)
                slot_ids(plus)
        for t in range(2):
            sib_wait(last_at - 1 + t, last_at - 1 + t, True)
            if t == 0:
                slot_ids(1)
            project([(slot, which, t) for slot, which, _ in farthest], (1, 3))
        for t in range(2):
            quarters = [(slot, which, t) for slot, which, _ in leading]
            attend(quarters)
            lead_send_all(t)
        project(farthest, (0, 1))
        attend(farthest)
        send_parts(farthest)
        rs_step(1, need)
        gather_end(True)
        attend(trailing)
        send_parts(trailing)
        for p in range(far - 2, 0, -1):
            for pieces in (both(2 * p), both(2 * p + 1)) + ((own,) if p == 1 else ()):
                attend(pieces)
                send_parts(pieces)
            rs_step(2 * (far - 1 - p), need)
            rs_step(2 * (far - 1 - p) + 1, need)
        rs_step(steps - 1, need)
        need_all(need)

    def mlp_half(layer):
        need = needs()

        def up(pieces):
            count_rows = rows * len(pieces)

            def body(c):
                cs = cols_at(c, utile)
                x = jnp.dot(load_rows(pieces), wup[:, cs], preferred_element_type=F32) + ub_ref[pl.ds(layer, 1), cs]
                inner = 0.7978845608028654 * (x + 0.044715 * (x * x * x))
                hidden[pl.ds(0, count_rows), cs] = (0.5 * x * (1.0 + jnp.tanh(inner))).astype(BF16)

            loop(units // utile, body)

        def down(pieces):
            count_rows = rows * len(pieces)
            step = min(wide, dim * 2 * rows // (2 * count_rows))

            def body(c):
                cs = cols_at(c, step)
                value = jnp.dot(hidden[pl.ds(0, count_rows), :], wdown[:, cs], preferred_element_type=F32).astype(BF16)
                store_part(pieces, value, cs)

            loop(dim // step, body)

        weight_copy(wup_hbm.at[layer], wup, 2).wait()
        weight_copy(wdown_hbm.at[layer], wdown, 3).wait()

        @pl.when(layer + 1 < layers)
        def _():
            weight_copy(wqkv_hbm.at[layer + 1], wqkv, 0).start()
            weight_copy(wout_hbm.at[layer + 1], wout, 1).start()

        for m in range(last_at):
            gather_step(m, False)
            if m == 0:
                own_wait(False)
                up(own)
            if m == 1:
                down(own)
                send_parts(own)
            for p in range(1, far - 2):
                if m == 4 * p:
                    sib_wait(4 * p - 4, 4 * p - 1, False)
                    up(near(p))
                if m == 4 * p + 1:
                    down(near(p))
                    send_parts(near(p))
            if m == lead_at:
                sib_wait(lead_at - 5, lead_at, False)
                up(leading)
                down(leading)
                for t in range(2):
                    lead_send_all(t)
        gather_step(last_at, False)
        sib_wait(lead_at + 1, last_at, False)
        up(farthest + trailing)
        down(farthest + trailing)
        send_parts(farthest + trailing)
        rs_step(1, need)
        gather_end(False)
        up(near(far - 2))
        down(near(far - 2))
        send_parts(near(far - 2))
        for m in range(2, steps):
            rs_step(m, need)
        need_all(need)

    weight_copy(wqkv_hbm.at[0], wqkv, 0).start()
    weight_copy(wout_hbm.at[0], wout, 1).start()
    barrier = pltpu.get_barrier_semaphore()
    for device in (left, right, sibling) + crossed:
        pl.semaphore_signal(barrier, inc=1, device_id={"tp": device}, device_id_type=MESH)
    hbuf[0, core, pl.ds(0, quarter), pl.ds(dim, ID_COLS)] = jnp.zeros((quarter, ID_COLS), BF16)
    hbuf[0, core, pl.ds(0, quarter), pl.ds(dim, rows)] = jnp.broadcast_to(ids_ref[...].astype(F32).astype(BF16), (quarter, rows))
    for slot in range(chips):
        kpos[:, pl.ds(slot * chip_rows, chip_rows)] = lax.broadcasted_iota(jnp.int32, (8, chip_rows), 1) + slot_chip(slot) * chip_rows
    for t in range(2):
        def widen(i, acc):
            out = []
            for which in range(2):
                rws = quarter_rows(which, t)
                value = tokens_ref[rws, cols_at(i, tile)].astype(F32)
                resid[rws, cols_at(i, tile)] = value
                out.append(acc[which] + value)
            return tuple(out)

        zero = jnp.zeros((quarter, tile), F32)
        sums = lax.fori_loop(0, dim // tile, widen, (zero, zero))
        norm_send(t, sums, 0, g1_ref, s1_ref, True, (lambda: pl.semaphore_wait(barrier, 5)) if t == 0 else None)

    def layer_body(layer):
        attention_half(layer)
        boundary(layer, ob_ref, layer, g2_ref, s2_ref, False)
        mlp_half(layer)
        boundary(layer, db_ref, lax.rem(layer + 1, layers), g1_ref, s1_ref, True, layer + 1 < layers)

    loop(layers, layer_body)


def solution(mesh):
    n = mesh.shape["tp"]
    chips = n // 2
    far = chips // 2
    steps = 2 * far - 1
    sends = 4 * far - 2
    row_spec = P("dp", "tp", None)
    vec_spec = P(None, None)
    in_specs = (row_spec, P("dp", "tp"), vec_spec, vec_spec, P(None, None, None, "tp", None), P(None, "tp", None, None), vec_spec, vec_spec, vec_spec, P(None, None, "tp"), P(None, "tp"), P(None, "tp", None), vec_spec)

    def device_fn(tokens, doc_ids, norm1_gain, norm1_shift, qkv_weight, out_weight, out_bias, norm2_gain, norm2_shift, up_weight, up_bias, down_weight, down_bias):
        batch, rows, dim = tokens.shape
        layers = norm1_gain.shape[0]
        head = qkv_weight.shape[-1]
        units = up_weight.shape[-1]
        wqkv = jnp.transpose(qkv_weight, (0, 2, 3, 1, 4)).reshape(layers, 3, dim, head)
        wout = out_weight.reshape(layers, head, dim)
        vmem = pl.BlockSpec(memory_space=pltpu.VMEM)
        hbm = pl.BlockSpec(memory_space=pl.ANY)
        dma = pltpu.SemaphoreType.DMA
        result = pl.pallas_call(
            functools.partial(block_kernel, n),
            out_shape=jax.ShapeDtypeStruct((rows, dim), BF16),
            in_specs=[vmem] * 9 + [hbm] * 4,
            out_specs=vmem,
            scratch_shapes=[
                pltpu.VMEM((chips, 2, rows, dim + ID_COLS), BF16),
                pltpu.VMEM((chips, 2, rows, dim), BF16),
                pltpu.VMEM((chips, rows, dim), BF16),
                pltpu.VMEM((2, steps, 2, rows // 4, dim), F32),
                pltpu.VMEM((2, 2, rows // 4, dim), F32),
                pltpu.VMEM((2, 2, 2, rows // 4, dim), BF16),
                pltpu.VMEM((rows, dim), F32),
                pltpu.VMEM((3, dim, head), BF16),
                pltpu.VMEM((head, dim), BF16),
                pltpu.VMEM((dim, units), BF16),
                pltpu.VMEM((units, dim), BF16),
                pltpu.VMEM((3, chips, 2, rows, head), BF16),
                pltpu.VMEM((4 * rows, units), BF16),
                pltpu.VMEM((8, chips * 2 * rows), jnp.int32),
                pltpu.VMEM((8, chips * 2 * rows), F32),
                dma((2, sends)), dma((2, sends)), dma((2, sends)), dma((2, sends)), dma((2, 2)), dma((2, 2)),
                dma((chips, 2, 2)), dma((chips, 2, 2)), dma((2, steps, 2)), dma((2, steps, 2)), dma((2, 2, 2)), dma((2, 2, 2)), dma((4,)),
            ],
            compiler_params=pltpu.CompilerParams(collective_id=0, has_side_effects=True, vmem_limit_bytes=67043328),
        )(tokens.reshape(rows, dim), doc_ids, norm1_gain, norm1_shift, out_bias, norm2_gain, norm2_shift, up_bias, down_bias, wqkv, wout, up_weight, down_weight)
        return result.reshape(batch, rows, dim)

    return jax.shard_map(device_fn, mesh=mesh, in_specs=in_specs, out_specs=row_spec, check_vma=False)
```

```python
import functools

import jax
import jax.numpy as jnp
from jax import lax
from jax.experimental import pallas as pl
from jax.experimental.pallas import tpu as pltpu
from jax.sharding import PartitionSpec as P

MESH = pl.DeviceIdType.MESH
F32, BF16 = jnp.float32, jnp.bfloat16
ID_COLS = 128
RIGHT, LEFT = 0, 1


def loop(count, body):
    lax.fori_loop(0, count, lambda i, carry: (body(i), carry)[1], 0)


def cols_at(i, width):
    return pl.ds(pl.multiple_of(i * width, width), width)


def block_kernel(n, tokens_ref, ids_ref, g1_ref, s1_ref, ob_ref, g2_ref, s2_ref, ub_ref, db_ref, wqkv_hbm, wout_hbm, wup_hbm, wdown_hbm,
                 out_ref, hbuf, part, psib, ring, fresh, lead, resid, wqkv, wout, wup, wdown, qkv, hidden, kpos, kids,
                 ag_send, ag_recv, sib_send, sib_recv, own_send, own_recv, part_send, part_recv, rs_send, rs_recv, lead_send, lead_recv, w_sem):
    chips = n // 2
    far = chips // 2
    steps = 2 * far - 1
    layers = g1_ref.shape[0]
    rows, dim = tokens_ref.shape
    half_rows, quarter = rows // 2, rows // 4
    chip_rows = 2 * rows
    head = wout.shape[0]
    units = wup.shape[1]
    tile = min(512, dim)
    utile = min(512, units)
    wide = min(2048, dim)

    me = lax.axis_index("tp")
    core = lax.rem(me, 2)
    chip = me // 2
    right, left = lax.rem(me + 2, n), lax.rem(me + n - 2, n)
    sibling = me + 1 - 2 * core
    target = (right, left)
    crossed = (right + 1 - 2 * core, left + 1 - 2 * core)

    def slot_of(offset):
        if offset == 0:
            return 0
        if abs(offset) == far:
            return 1
        return 2 * abs(offset) + (1 if offset > 0 else 0)

    def slot_chip(slot):
        if slot == 0:
            return chip
        if slot == 1:
            return lax.rem(chip + far, chips)
        offset = slot // 2 if slot % 2 else -(slot // 2)
        return lax.rem(chip + chips + offset, chips)

    def signed(direction, distance):
        return -distance if direction == RIGHT else distance

    def quarter_rows(which, t):
        return pl.ds(which * half_rows + t * quarter, quarter)

    def half_ds(which):
        return pl.ds(which * half_rows, half_rows)

    def messages(direction):
        a, b = direction, 1 - direction
        out = [(0, a, 0), (0, b, 0), (0, a, 1), (0, b, 1)]
        for j in range(1, far - 1):
            out += [(j, a, 0), (j, a, 1), (j, b, 0), (j, b, 1)]
        return out + [(far - 1, a, 0), (far - 1, a, 1)]

    plans = (messages(RIGHT), messages(LEFT))
    count = len(plans[0])

    def width_of(which, t, with_ids):
        return dim + ID_COLS if with_ids and which == 0 and t == 0 else dim

    def ag_ref(direction, m, extra, with_ids):
        j, which, t = plans[direction][m]
        return hbuf.at[slot_of(signed(direction, j + extra)), core, quarter_rows(which, t), pl.ds(0, width_of(which, t, with_ids))]

    def ag_copy(direction, m, with_ids):
        return pltpu.make_async_remote_copy(
            src_ref=ag_ref(direction, m, 0, with_ids), dst_ref=ag_ref(direction, m, 1, with_ids),
            send_sem=ag_send.at[direction, m], recv_sem=ag_recv.at[direction, m],
            device_id={"tp": target[direction]}, device_id_type=MESH)

    def sib_copy(direction, m, with_ids):
        ref = ag_ref(direction, m, 1, with_ids)
        return pltpu.make_async_remote_copy(
            src_ref=ref, dst_ref=ref, send_sem=sib_send.at[direction, m], recv_sem=sib_recv.at[direction, m],
            device_id={"tp": sibling}, device_id_type=MESH)

    def own_copy(which, t, with_ids):
        ref = hbuf.at[0, core, quarter_rows(which, t), pl.ds(0, width_of(which, t, with_ids))]
        return pltpu.make_async_remote_copy(
            src_ref=ref, dst_ref=ref, send_sem=own_send.at[which, t], recv_sem=own_recv.at[which, t],
            device_id={"tp": sibling}, device_id_type=MESH)

    def part_copy(slot, which, t):
        rws = quarter_rows(which, t)
        return pltpu.make_async_remote_copy(
            src_ref=part.at[slot, 1 - core, rws], dst_ref=psib.at[slot, rws],
            send_sem=part_send.at[slot, which, t], recv_sem=part_recv.at[slot, which, t],
            device_id={"tp": sibling}, device_id_type=MESH)

    def rs_plan(direction, m):
        if m == steps - 1:
            which, distance, before = 0, 1, m - 1
        elif m % 2 == 0:
            which, distance, before = 1, far - 1 - m // 2, m - 2
        else:
            which, distance, before = 0, far - m // 2, m - 2
        dest = slot_of(-signed(direction, distance))
        return which ^ direction, dest, (before if m >= 2 else None)

    def rs_copy(direction, m, t):
        before = rs_plan(direction, m)[2]
        src = fresh.at[direction, t] if before is None else ring.at[direction, before, t]
        return pltpu.make_async_remote_copy(
            src_ref=src, dst_ref=ring.at[direction, m, t], send_sem=rs_send.at[direction, m, t], recv_sem=rs_recv.at[direction, m, t],
            device_id={"tp": target[direction]}, device_id_type=MESH)

    def lead_copy(direction, t, cross):
        which, dest, _ = rs_plan(direction, 0)
        return pltpu.make_async_remote_copy(
            src_ref=part.at[dest, 1 - core if cross else core, quarter_rows(which, t)], dst_ref=lead.at[direction, t, cross],
            send_sem=lead_send.at[direction, t, cross], recv_sem=lead_recv.at[direction, t, cross],
            device_id={"tp": (crossed if cross else target)[direction]}, device_id_type=MESH)

    def lead_send_all(t):
        for cross in (0, 1):
            for direction in (RIGHT, LEFT):
                lead_copy(direction, t, cross).start()

    def sum_send(m, t, need):
        for direction in (RIGHT, LEFT):
            which, dest, before = rs_plan(direction, m)
            need(dest, which, t)
            if before == 0:
                for cross in (0, 1):
                    lead_copy(direction, t, cross).wait_recv()
            elif before is not None:
                rs_copy(direction, before, t).wait_recv()
            rws = quarter_rows(which, t)

            def add(i):
                cs = cols_at(i, tile)
                total = part[dest, core, rws, cs].astype(F32) + psib[dest, rws, cs].astype(F32)
                if before is None:
                    fresh[direction, t, :, cs] = total
                elif before == 0:
                    first = lead[direction, t, 0, :, cs].astype(F32) + lead[direction, t, 1, :, cs].astype(F32)
                    ring[direction, 0, t, :, cs] = first + total
                else:
                    ring[direction, before, t, :, cs] = ring[direction, before, t, :, cs] + total

            loop(dim // tile, add)
            rs_copy(direction, m, t).start()

    def rs_step(m, need):
        for t in range(2):
            sum_send(m, t, need)

    def weight_copy(src, dst, index):
        return pltpu.make_async_copy(src, dst, w_sem.at[index])

    def norm_send(t, sums, layer, gain_ref, shift_ref, with_ids, before_send=None):
        means = [jnp.sum(s, axis=1, keepdims=True) / dim for s in sums]

        def sq_body(i, acc):
            out = []
            for which in range(2):
                centered = resid[quarter_rows(which, t), cols_at(i, tile)] - means[which]
                out.append(acc[which] + centered * centered)
            return tuple(out)

        zero = jnp.zeros((quarter, tile), F32)
        squares = lax.fori_loop(0, dim // tile, sq_body, (zero, zero))
        scales = [lax.rsqrt(jnp.sum(s, axis=1, keepdims=True) / dim + 1e-5) for s in squares]

        def out_body(i):
            cs = cols_at(i, tile)
            for which in range(2):
                rws = quarter_rows(which, t)
                value = (resid[rws, cs] - means[which]) * scales[which] * gain_ref[pl.ds(layer, 1), cs] + shift_ref[pl.ds(layer, 1), cs]
                hbuf[0, core, rws, cs] = value.astype(BF16)

        loop(dim // tile, out_body)
        if before_send is not None:
            before_send()
        for i in range(2):
            for direction in (RIGHT, LEFT):
                ag_copy(direction, 2 * t + i, with_ids).start()
        for which in range(2):
            own_copy(which, t, with_ids).start()

    def finish(t, layer, bias_ref):
        for which in range(2):
            rs_copy(1 - which, steps - 3, t).wait_recv()
            rs_copy(which, steps - 1, t).wait_recv()

        def body(i, acc):
            cs = cols_at(i, tile)
            out = []
            for which in range(2):
                rws = quarter_rows(which, t)
                total = part[0, core, rws, cs].astype(F32) + psib[0, rws, cs].astype(F32)
                total = total + ring[1 - which, steps - 3, t, :, cs] + ring[which, steps - 1, t, :, cs]
                value = resid[rws, cs] + (total + bias_ref[pl.ds(layer, 1), cs])
                resid[rws, cs] = value
                out_ref[rws, cs] = value.astype(BF16)
                out.append(acc[which] + value)
            return tuple(out)

        zero = jnp.zeros((quarter, tile), F32)
        return lax.fori_loop(0, dim // tile, body, (zero, zero))

    def boundary(layer, bias_ref, next_layer, gain_ref, shift_ref, with_ids, more=None):
        for t in range(2):
            sums = finish(t, layer, bias_ref)
            if more is None:
                norm_send(t, sums, next_layer, gain_ref, shift_ref, with_ids)
            else:
                @pl.when(more)
                def _():
                    norm_send(t, sums, next_layer, gain_ref, shift_ref, with_ids)
        for direction in (RIGHT, LEFT):
            for t in range(2):
                for cross in (0, 1):
                    lead_copy(direction, t, cross).wait_send()
                for m in range(1, steps):
                    rs_copy(direction, m, t).wait_send()
        for piece in exchanged:
            part_copy(*piece).wait_send()

    def needs():
        seen = set()

        def need(*piece):
            if piece not in seen:
                seen.add(piece)
                part_copy(*piece).wait_recv()

        return need

    def need_all(need):
        for piece in exchanged:
            need(*piece)

    def gather_step(m, with_ids):
        for direction in (RIGHT, LEFT):
            ag_copy(direction, m, with_ids).wait_recv()
            j, which, t = plans[direction][m]
            if (j + 1, which, t) in plans[direction]:
                ag_copy(direction, plans[direction].index((j + 1, which, t)), with_ids).start()
            sib_copy(direction, m, with_ids).start()

    def sib_wait(first, last, with_ids):
        for m in range(first, last + 1):
            for direction in (RIGHT, LEFT):
                sib_copy(direction, m, with_ids).wait_recv()

    def own_wait(with_ids):
        for which in range(2):
            for t in range(2):
                own_copy(which, t, with_ids).wait_recv()

    def gather_end(with_ids):
        for which in range(2):
            for t in range(2):
                own_copy(which, t, with_ids).wait_send()
        for m in range(count):
            for direction in (RIGHT, LEFT):
                ag_copy(direction, m, with_ids).wait_send()
                sib_copy(direction, m, with_ids).wait_send()

    def piece_rows(piece):
        slot, which, t = piece
        return half_ds(which) if t is None else quarter_rows(which, t)

    def piece_size(piece):
        return rows if piece[2] is None else half_rows

    def load_rows(pieces):
        return jnp.concatenate([hbuf[p[0], :, piece_rows(p), pl.ds(0, dim)].reshape(piece_size(p), dim) for p in pieces], axis=0)

    def store_part(pieces, value, cs):
        start = 0
        for p in pieces:
            size = piece_size(p)
            part[p[0], :, piece_rows(p), cs] = value[start:start + size].reshape(2, size // 2, value.shape[1])
            start += size

    def both(slot):
        return [(slot, 0, None), (slot, 1, None)]

    minus, plus = slot_of(-(far - 1)), slot_of(far - 1)
    own = both(0)
    farthest = both(1)
    leading = [(minus, 0, None), (plus, 1, None)]
    trailing = [(minus, 1, None), (plus, 0, None)]

    exchanged = [(slot, which, t) for slot in range(chips) for which in range(2) for t in range(2) if (slot, which, None) not in leading]

    def near(p):
        return both(2 * p) + both(2 * p + 1)

    lead_at = 4 * (far - 2) + 1
    last_at = count - 1

    def send_parts(pieces):
        for slot, which, t in pieces:
            for u in range(2) if t is None else (t,):
                part_copy(slot, which, u).start()

    def attention_half(layer):
        need = needs()

        def project(pieces, kinds=(0, 3)):
            def body(t):
                value = jnp.dot(load_rows(pieces), wqkv[t], preferred_element_type=F32).astype(BF16)
                start = 0
                for p in pieces:
                    size = piece_size(p)
                    qkv[t, p[0], :, piece_rows(p)] = value[start:start + size].reshape(2, size // 2, head)
                    start += size

            lax.fori_loop(kinds[0], kinds[1], lambda t, carry: (body(t), carry)[1], 0)

        def slot_ids(slot):
            cs = pl.ds(slot * chip_rows, chip_rows)
            lines = [hbuf[slot, c, pl.ds(0, 8), pl.ds(dim, ID_COLS)].astype(F32)[:, 0:rows] for c in range(2)]
            kids[:, cs] = jnp.concatenate(lines, axis=1)

        def column_ids(piece):
            line = kids[0:1, pl.ds(piece[0] * chip_rows, chip_rows)]
            column = jnp.broadcast_to(line, (chip_rows, chip_rows)).T[:, 0:1]
            size = piece_size(piece) // 2
            first = piece[1] * half_rows + (piece[2] or 0) * quarter
            return jnp.concatenate([column[c * rows + first:c * rows + first + size] for c in range(2)], axis=0)

        def column_pos(piece):
            size = piece_size(piece) // 2
            first = piece[1] * half_rows + (piece[2] or 0) * quarter
            i = lax.broadcasted_iota(jnp.int32, (2 * size, 1), 0)
            i = i + jnp.where(i >= size, rows - size, 0)
            return i + (first + slot_chip(piece[0]) * chip_rows)

        def attend(pieces):
            keys = qkv[1].reshape(chips * chip_rows, head)
            values = qkv[2].reshape(chips * chip_rows, head)
            queries = jnp.concatenate([qkv[0, p[0], :, piece_rows(p)].reshape(piece_size(p), head) for p in pieces], axis=0)
            scores = lax.dot_general(queries, keys, (((1,), (1,)), ((), ())), preferred_element_type=F32) * (head ** -0.5)
            ids_col = jnp.concatenate([column_ids(piece) for piece in pieces], axis=0)
            pos_col = jnp.concatenate([column_pos(piece) for piece in pieces], axis=0)
            allowed = (kpos[0:1, :] <= pos_col) & (kids[0:1, :] == ids_col)
            scores = jnp.where(allowed, scores, -1e30)
            top = jnp.max(scores, axis=1, keepdims=True)
            probs = jnp.exp(scores - top)
            probs = (probs * (1.0 / jnp.sum(probs, axis=1, keepdims=True))).astype(BF16)
            mixed = jnp.dot(probs, values, preferred_element_type=F32).astype(BF16)

            def proj(c):
                cs = cols_at(c, wide)
                store_part(pieces, jnp.dot(mixed, wout[:, cs], preferred_element_type=F32).astype(BF16), cs)

            loop(dim // wide, proj)

        weight_copy(wup_hbm.at[layer], wup, 2).start()
        weight_copy(wdown_hbm.at[layer], wdown, 3).start()
        weight_copy(wqkv_hbm.at[layer], wqkv, 0).wait()
        weight_copy(wout_hbm.at[layer], wout, 1).wait()
        for m in range(count):
            gather_step(m, True)
            if m == 0:
                own_wait(True)
                project(own)
                slot_ids(0)
            for p in range(1, far - 1):
                if m == 4 * p:
                    sib_wait(4 * p - 4, 4 * p - 1, True)
                    project(near(p))
                    slot_ids(2 * p)
                    slot_ids(2 * p + 1)
            if m == last_at - 2:
                sib_wait(lead_at - 1, m, True)
                project(leading + trailing)
                slot_ids(minus)
                slot_ids(plus)
        for t in range(2):
            sib_wait(last_at - 1 + t, last_at - 1 + t, True)
            if t == 0:
                slot_ids(1)
            project([(slot, which, t) for slot, which, _ in farthest], (1, 3))
        for t in range(2):
            quarters = [(slot, which, t) for slot, which, _ in leading]
            attend(quarters)
            lead_send_all(t)
        project(farthest, (0, 1))
        attend(farthest)
        send_parts(farthest)
        rs_step(1, need)
        gather_end(True)
        attend(trailing)
        send_parts(trailing)
        for p in range(far - 2, 0, -1):
            for pieces in (both(2 * p), both(2 * p + 1)) + ((own,) if p == 1 else ()):
                attend(pieces)
                send_parts(pieces)
            rs_step(2 * (far - 1 - p), need)
            rs_step(2 * (far - 1 - p) + 1, need)
        rs_step(steps - 1, need)
        need_all(need)

    def mlp_half(layer):
        need = needs()

        def up(pieces):
            count_rows = rows * len(pieces)

            def body(c):
                cs = cols_at(c, utile)
                x = jnp.dot(load_rows(pieces), wup[:, cs], preferred_element_type=F32) + ub_ref[pl.ds(layer, 1), cs]
                inner = 0.7978845608028654 * (x + 0.044715 * (x * x * x))
                hidden[pl.ds(0, count_rows), cs] = (0.5 * x * (1.0 + jnp.tanh(inner))).astype(BF16)

            loop(units // utile, body)

        def down(pieces):
            count_rows = rows * len(pieces)
            step = min(wide, dim * 2 * rows // (2 * count_rows))

            def body(c):
                cs = cols_at(c, step)
                value = jnp.dot(hidden[pl.ds(0, count_rows), :], wdown[:, cs], preferred_element_type=F32).astype(BF16)
                store_part(pieces, value, cs)

            loop(dim // step, body)

        weight_copy(wup_hbm.at[layer], wup, 2).wait()
        weight_copy(wdown_hbm.at[layer], wdown, 3).wait()

        @pl.when(layer + 1 < layers)
        def _():
            weight_copy(wqkv_hbm.at[layer + 1], wqkv, 0).start()
            weight_copy(wout_hbm.at[layer + 1], wout, 1).start()

        for m in range(last_at):
            gather_step(m, False)
            if m == 0:
                own_wait(False)
                up(own)
            if m == 1:
                down(own)
                send_parts(own)
            for p in range(1, far - 2):
                if m == 4 * p:
                    sib_wait(4 * p - 4, 4 * p - 1, False)
                    up(near(p))
                if m == 4 * p + 1:
                    down(near(p))
                    send_parts(near(p))
            if m == lead_at:
                sib_wait(lead_at - 5, lead_at, False)
                up(leading)
                down(leading)
                for t in range(2):
                    lead_send_all(t)
        gather_step(last_at, False)
        sib_wait(lead_at + 1, last_at, False)
        up(farthest)
        down(farthest)
        send_parts(farthest)
        rs_step(1, need)
        up(near(far - 2))
        down(near(far - 2))
        send_parts(near(far - 2))
        gather_end(False)
        up(trailing)
        down(trailing)
        send_parts(trailing)
        for m in range(2, steps):
            rs_step(m, need)
        need_all(need)

    weight_copy(wqkv_hbm.at[0], wqkv, 0).start()
    weight_copy(wout_hbm.at[0], wout, 1).start()
    barrier = pltpu.get_barrier_semaphore()
    for device in (left, right, sibling) + crossed:
        pl.semaphore_signal(barrier, inc=1, device_id={"tp": device}, device_id_type=MESH)
    hbuf[0, core, pl.ds(0, quarter), pl.ds(dim, ID_COLS)] = jnp.zeros((quarter, ID_COLS), BF16)
    hbuf[0, core, pl.ds(0, quarter), pl.ds(dim, rows)] = jnp.broadcast_to(ids_ref[...].astype(F32).astype(BF16), (quarter, rows))
    for slot in range(chips):
        kpos[:, pl.ds(slot * chip_rows, chip_rows)] = lax.broadcasted_iota(jnp.int32, (8, chip_rows), 1) + slot_chip(slot) * chip_rows
    for t in range(2):
        def widen(i, acc):
            out = []
            for which in range(2):
                rws = quarter_rows(which, t)
                value = tokens_ref[rws, cols_at(i, tile)].astype(F32)
                resid[rws, cols_at(i, tile)] = value
                out.append(acc[which] + value)
            return tuple(out)

        zero = jnp.zeros((quarter, tile), F32)
        sums = lax.fori_loop(0, dim // tile, widen, (zero, zero))
        norm_send(t, sums, 0, g1_ref, s1_ref, True, (lambda: pl.semaphore_wait(barrier, 5)) if t == 0 else None)

    def layer_body(layer):
        attention_half(layer)
        boundary(layer, ob_ref, layer, g2_ref, s2_ref, False)
        mlp_half(layer)
        boundary(layer, db_ref, lax.rem(layer + 1, layers), g1_ref, s1_ref, True, layer + 1 < layers)

    loop(layers, layer_body)


def solution(mesh):
    n = mesh.shape["tp"]
    chips = n // 2
    far = chips // 2
    steps = 2 * far - 1
    sends = 4 * far - 2
    row_spec = P("dp", "tp", None)
    vec_spec = P(None, None)
    in_specs = (row_spec, P("dp", "tp"), vec_spec, vec_spec, P(None, None, None, "tp", None), P(None, "tp", None, None), vec_spec, vec_spec, vec_spec, P(None, None, "tp"), P(None, "tp"), P(None, "tp", None), vec_spec)

    def device_fn(tokens, doc_ids, norm1_gain, norm1_shift, qkv_weight, out_weight, out_bias, norm2_gain, norm2_shift, up_weight, up_bias, down_weight, down_bias):
        batch, rows, dim = tokens.shape
        layers = norm1_gain.shape[0]
        head = qkv_weight.shape[-1]
        units = up_weight.shape[-1]
        wqkv = jnp.transpose(qkv_weight, (0, 2, 3, 1, 4)).reshape(layers, 3, dim, head)
        wout = out_weight.reshape(layers, head, dim)
        vmem = pl.BlockSpec(memory_space=pltpu.VMEM)
        hbm = pl.BlockSpec(memory_space=pl.ANY)
        dma = pltpu.SemaphoreType.DMA
        result = pl.pallas_call(
            functools.partial(block_kernel, n),
            out_shape=jax.ShapeDtypeStruct((rows, dim), BF16),
            in_specs=[vmem] * 9 + [hbm] * 4,
            out_specs=vmem,
            scratch_shapes=[
                pltpu.VMEM((chips, 2, rows, dim + ID_COLS), BF16),
                pltpu.VMEM((chips, 2, rows, dim), BF16),
                pltpu.VMEM((chips, rows, dim), BF16),
                pltpu.VMEM((2, steps, 2, rows // 4, dim), F32),
                pltpu.VMEM((2, 2, rows // 4, dim), F32),
                pltpu.VMEM((2, 2, 2, rows // 4, dim), BF16),
                pltpu.VMEM((rows, dim), F32),
                pltpu.VMEM((3, dim, head), BF16),
                pltpu.VMEM((head, dim), BF16),
                pltpu.VMEM((dim, units), BF16),
                pltpu.VMEM((units, dim), BF16),
                pltpu.VMEM((3, chips, 2, rows, head), BF16),
                pltpu.VMEM((4 * rows, units), BF16),
                pltpu.VMEM((8, chips * 2 * rows), jnp.int32),
                pltpu.VMEM((8, chips * 2 * rows), F32),
                dma((2, sends)), dma((2, sends)), dma((2, sends)), dma((2, sends)), dma((2, 2)), dma((2, 2)),
                dma((chips, 2, 2)), dma((chips, 2, 2)), dma((2, steps, 2)), dma((2, steps, 2)), dma((2, 2, 2)), dma((2, 2, 2)), dma((4,)),
            ],
            compiler_params=pltpu.CompilerParams(collective_id=0, has_side_effects=True, vmem_limit_bytes=67043328),
        )(tokens.reshape(rows, dim), doc_ids, norm1_gain, norm1_shift, out_bias, norm2_gain, norm2_shift, up_bias, down_bias, wqkv, wout, up_weight, down_weight)
        return result.reshape(batch, rows, dim)

    return jax.shard_map(device_fn, mesh=mesh, in_specs=in_specs, out_specs=row_spec, check_vma=False)
```
